512 devices in a mesh: frames: 32 (over x_lo, z), blocks: 16 (over x_hi, y, core).
Axes of the slice: x: 4 (x_hi: 2, x_lo: 2; x = x_hi * 2 + x_lo), y: 4, z: 16, core: 2. Of those that a mesh axis runs over, the one named last changes fastest.
Arguments:
- frames_data: bfloat16 [114688, 2048], P('frames', 'blocks'), may hold values from -8 to 14
- traj_ids: int32 [114688], P('frames'), may hold values from 0 to 255, never falling along the last dimension, each value on 1 to 7168 neighbouring positions
Outputs:
- cov_zero: float32 [2048, 2048], P('frames', 'blocks')
- cov_lag: float32 [2048, 2048], P('frames', 'blocks')
The draws below stay inside these ranges and needn't reach their ends.
Inputs may be any that keep to these rules, and one draw needn't show every extreme that they name: `traj_ids`: ids never fall along the frames; each trajectory is a contiguous run of 1 to 7168 frames and some trajectory has exactly 7168.
All inputs are finite; a program needn't handle non-finite values.
Results may differ from the reference program's by a relative error of at most 0.0003.
Values may be sent and summed in bfloat16 or wider, within the bound.
No kernel may reach another device: no remote copies, remote signals or barrier semaphores. Data moves between devices by JAX's collectives and lax.ppermute only.
A program may use at most 64 MiB of HBM per device.

```python
import math
import jax
import jax.numpy as jnp
import numpy as np
from jax import lax

F = 2048
LAG = 64
FRAMES = 114688
NTRAJ = 256
MAXLEN = 7168


def draw_frames_data(key, part):
    key_mean = jax.random.fold_in(key, 11)
    key_now = jax.random.fold_in(key, 12)
    offsets = jax.random.uniform(key_mean, (F,), jnp.float32, 0.5, 2.0)
    position = jnp.arange(FRAMES, dtype=jnp.float32) / max(FRAMES - 1, 1)
    rising = 0.5 + position
    fresh_noise = jnp.clip(jax.random.normal(key_now, (FRAMES + LAG, F), jnp.float32), -5.0, 5.0)
    noise_rows = fresh_noise[LAG:] + 0.7 * fresh_noise[:FRAMES]
    values = offsets[None, :] * rising[:, None] + noise_rows
    return jnp.clip(values, -8.0, 14.0).astype(jnp.bfloat16)


def profile(number_of, total, limit, slope):
    portions = [(1 << 20) // math.isqrt(rank ** slope) + 1 for rank in range(2, number_of + 1)]
    rest, counts = total - limit - (number_of - 1), [1] * (number_of - 1)
    while rest > 0:
        movable = [i for i in range(number_of - 1) if counts[i] < limit]
        mass, left = sum([portions[i] for i in movable]), rest
        for i in movable:
            addition = min(limit - counts[i], max(1, left * portions[i] // mass), rest)
            counts[i] = counts[i] + addition
            rest = rest - addition
    return np.array([limit] + counts)


def uneven(rng, amount, total, limit, lean):
    if amount == 2:
        one = jax.random.randint(rng, (), max(1, total - limit), min(limit, total - 1) + 1)
        return jnp.stack([one, total - one])
    lengths = jnp.asarray(profile(amount, total, limit, lean), jnp.int32)
    couples = (amount - 1) // 2
    source_of, taker = lengths[1:1 + 2 * couples:2], lengths[2:2 + 2 * couples:2]
    slack = jnp.minimum(source_of - 1, limit - taker)
    moved = jax.random.randint(jax.random.fold_in(rng, 1), (couples,), 0, 1 << 20) % (slack + 1)
    lengths = lengths.at[1:1 + 2 * couples:2].set(source_of - moved).at[2:2 + 2 * couples:2].set(taker + moved)
    return lengths[jax.random.permutation(jax.random.fold_in(rng, 2), amount)]


def setup_inputs(seed: int = 0) -> dict:
    splits = jax.random.split(jax.random.key(seed), 3)
    return {
        "frames_data": draw_frames_data(jax.random.fold_in(splits[2], 71), 0),
        "traj_ids": jnp.searchsorted(jnp.cumsum(uneven(splits[1], NTRAJ, FRAMES, MAXLEN, 2)), jnp.arange(FRAMES), side="right").astype(jnp.int32),
    }


def reference(frames_data, traj_ids):
    ahead = jnp.concatenate([traj_ids[LAG:] + 1, jnp.zeros((LAG,), jnp.int32)])
    valid = ahead == traj_ids + 1
    zeros = jnp.zeros_like(frames_data)
    current = jnp.where(valid[:, None], frames_data, zeros)
    later = jnp.concatenate([frames_data[LAG:], jnp.zeros((LAG, F), frames_data.dtype)], axis=0)
    count = jnp.sum(valid.astype(jnp.float32))
    mean_zero = jnp.sum(current.astype(jnp.float32), axis=0) / count
    mean_lag = jnp.sum(jnp.where(valid[:, None], later, zeros).astype(jnp.float32), axis=0) / count
    plain = lax.dot_general(current, current, (((0,), (0,)), ((), ())), preferred_element_type=jnp.float32)
    lagged = lax.dot_general(current, later, (((0,), (0,)), ((), ())), preferred_element_type=jnp.float32)
    cov_zero = plain / count - mean_zero[:, None] * mean_zero[None, :]
    cov_lag = lagged / count - mean_zero[:, None] * mean_lag[None, :]
    return cov_zero, cov_lag
```

```python
import jax
import jax.numpy as jnp
from jax import lax
from jax.sharding import PartitionSpec as P


LAG = 64
AXES = ("frames", "blocks")


def pairs(move):
    out = []
    for frame in range(32):
        for block in range(16):
            target = move(frame // 16, frame % 16, block // 8, (block // 2) % 4, block % 2)
            if target is None:
                continue
            xl, z, xh, y, c = target
            out.append((frame * 16 + block, (xl * 16 + z % 16) * 16 + xh * 8 + (y % 4) * 2 + c))
    return out


def send(value, move):
    return lax.ppermute(value, AXES, pairs(move))


def to_previous(xl, z, xh, y, c):
    frame = xl * 16 + z - 1
    return None if frame < 0 else (frame // 16, frame % 16, xh, y, c)


def along_y(step):
    return lambda xl, z, xh, y, c: (xl, z, xh, y - step, c)


def swap_x_hi(xl, z, xh, y, c):
    return (xl, z, 1 - xh, y, c)


def swap_core(xl, z, xh, y, c):
    return (xl, z, xh, y, 1 - c)


def swap_x_lo(xl, z, xh, y, c):
    return (1 - xl, z, xh, y, c)


def near(step):
    return lambda xl, z, xh, y, c: (xl, z ^ step, xh, y, c)


def near_shifted(step):
    return lambda xl, z, xh, y, c: (xl, z + step if z & step else z - step, xh, y, c)


def to_owner(step):
    def move(xl, z, xh, y, c):
        high, bit1, bit0 = (z // 4 + step) % 4, (z // 2) % 2, z % 2
        return (xh, high * 4 + c * 2 + bit1, xl, y, bit0)

    return move


def contract(left, right):
    return lax.dot_general(left, right, (((0,), (0,)), ((), ())), preferred_element_type=jnp.float32)


def shards(frames_data, traj_ids):
    frame, block = lax.axis_index("frames"), lax.axis_index("blocks")
    x_lo, z = frame // 16, frame % 16
    x_hi, y, core = block // 8, (block // 2) % 4, block % 2
    z_high, bit1, bit0 = z // 4, (z // 2) % 2, z % 2

    own = frames_data
    rows = own.shape[0]
    marks = traj_ids + 1
    side = [own] + [send(own, along_y(k)) for k in (1, 2, 3)]
    over_x = send(own, swap_x_hi)
    over_core = send(own, swap_core)
    rim = send(marks[:LAG], to_previous)
    over_both = send(over_x, swap_core)

    valid = jnp.concatenate([marks[LAG:], rim]) == marks
    left = [jnp.where(valid[:, None], part, jnp.zeros_like(part)) for part in side]
    weight = jnp.broadcast_to(valid.astype(jnp.bfloat16)[:, None], (rows, 8))
    sums_left = jnp.stack([contract(weight, part)[:1] for part in left])
    left = jnp.concatenate(left + [weight], axis=1)

    same_x, same_c = x_lo == x_hi, bit0 == core

    def ordered(blocks):
        mine, core_side, x_side, both = blocks
        near_k, far_k = jnp.where(same_x, mine, x_side), jnp.where(same_x, core_side, both)
        near_s, far_s = jnp.where(same_x, x_side, mine), jnp.where(same_x, both, core_side)
        return (
            jnp.where(same_c, near_k, far_k),
            jnp.where(same_c, far_k, near_k),
            jnp.where(same_c, near_s, far_s),
            jnp.where(same_c, far_s, near_s),
        )

    gathered = (own, over_core, over_x, over_both)
    rims = jnp.concatenate([part[:LAG] for part in gathered], axis=1)
    halo = ordered(jnp.split(send(rims, to_previous), 4, axis=1))
    right = ordered(gathered)
    ahead = [jnp.concatenate([part[LAG:], tip], axis=0) for part, tip in zip(right, halo)]
    products = contract(left, jnp.concatenate(right, axis=1))
    later = contract(left, jnp.concatenate([ahead[0], ahead[2], ahead[1], ahead[3]], axis=1))

    plain = products[:512].reshape(4, 2, LAG, 512)
    lagged = later[:512].reshape(4, 2, LAG, 512)
    sums_later = later[512]
    sums_later = jnp.concatenate([sums_later[:128], sums_later[256:384], sums_later[128:256], sums_later[384:]])
    count_here = jnp.sum(valid.astype(jnp.float32))
    extra = jnp.concatenate(
        [
            jnp.broadcast_to(products[512][None, None, :], (4, 1, 512)),
            jnp.broadcast_to(sums_later[None, None, :], (4, 1, 512)),
            jnp.tile(sums_left, (1, 1, 4)),
            jnp.broadcast_to(count_here, (4, 5, 512)),
        ],
        axis=1,
    )
    plain = jnp.concatenate([plain, jnp.broadcast_to(extra[:, None], (4, 2, 8, 512))], axis=2)

    plain = plain[..., :256] + send(plain[..., 256:], swap_x_lo)
    lagged = lagged[..., :256] + send(lagged[..., 256:], near_shifted(1))
    plain = plain[..., :128] + send(plain[..., 128:], near(1))
    lagged = lagged[..., :128] + send(lagged[..., 128:], swap_x_lo)

    def half(value, index):
        return lax.dynamic_index_in_dim(value, index, 1, keepdims=False)

    plain = half(plain, bit1) + send(half(plain, 1 - bit1), near(2))
    lagged = half(lagged, bit1) + send(half(lagged, 1 - bit1), near_shifted(2))
    pieces = jnp.concatenate([plain, lagged], axis=1)

    total = 0.0
    for step in range(4):
        piece = lax.dynamic_index_in_dim(pieces, (z_high + step - y) % 4, 0, keepdims=False)
        total = total + send(piece, to_owner(step))

    count = total[LAG + 3, 0]
    mean_cols, lag_cols = total[LAG] / count, total[LAG + 1] / count
    mean_rows = lax.dynamic_slice_in_dim(total[LAG + 2], bit0 * LAG, LAG, 0) / count
    cov_zero = total[:LAG] / count - mean_rows[:, None] * mean_cols[None, :]
    cov_lag = total[LAG + 8 :] / count - mean_rows[:, None] * lag_cols[None, :]
    return (cov_zero, cov_lag)


def solution(mesh):
    return jax.shard_map(
        shards,
        mesh=mesh,
        in_specs=(P("frames", "blocks"), P("frames")),
        out_specs=(P("frames", "blocks"), P("frames", "blocks")),
        check_vma=False,
    )
```

```python
import functools

import jax
import jax.numpy as jnp
from jax import lax
from jax.experimental import pallas as pl
from jax.experimental.pallas import tpu as pltpu
from jax.sharding import PartitionSpec as P


LAG = 64
AXES = ("frames", "blocks")


def pairs(move):
    out = []
    for frame in range(32):
        for block in range(16):
            target = move(frame // 16, frame % 16, block // 8, (block // 2) % 4, block % 2)
            if target is None:
                continue
            xl, z, xh, y, c = target
            out.append((frame * 16 + block, (xl * 16 + z % 16) * 16 + xh * 8 + (y % 4) * 2 + c))
    return out


def send(value, move):
    return lax.ppermute(value, AXES, pairs(move))


def to_previous(xl, z, xh, y, c):
    frame = xl * 16 + z - 1
    return None if frame < 0 else (frame // 16, frame % 16, xh, y, c)


def up_y(xl, z, xh, y, c):
    return (xl, z, xh, y + 1, c)


def down_y(xl, z, xh, y, c):
    return (xl, z, xh, y - 1, c)


def swap_x_hi(xl, z, xh, y, c):
    return (xl, z, 1 - xh, y, c)


def swap_core(xl, z, xh, y, c):
    return (xl, z, xh, y, 1 - c)


def swap_x_lo(xl, z, xh, y, c):
    return (1 - xl, z, xh, y, c)


def near(step):
    return lambda xl, z, xh, y, c: (xl, z ^ step, xh, y, c)


def near_shifted(step):
    return lambda xl, z, xh, y, c: (xl, z + step if z & step else z - step, xh, y, c)


def to_owner(step):
    def move(xl, z, xh, y, c):
        high, bit1, bit0 = (z // 4 + step) % 4, (z // 2) % 2, z % 2
        return (xh, high * 4 + c * 2 + bit0, xl, y, bit1)

    return move


def contract(left, right):
    return lax.dot_general(left, right, (((0,), (0,)), ((), ())), preferred_element_type=jnp.float32)


def spread_kernel(with_mask, first_ref, second_ref, mask_ref, low_ref, high_ref):
    middle, chunk = low_ref.shape[0], 256
    for part, out_ref in enumerate((low_ref, high_ref)):

        def body(i, carry, part=part, out_ref=out_ref):
            at = pl.multiple_of(i * chunk, chunk)
            start = pl.multiple_of(at + part * middle, chunk)
            mask = mask_ref[pl.ds(start, chunk), :]
            for column, ref in enumerate((first_ref, second_ref)):
                lanes, later = pl.ds(column * 128, 128), pl.ds(256 + column * 128, 128)
                out_ref[pl.ds(at, chunk), lanes] = ref[pl.ds(start, chunk), :] * mask
                out_ref[pl.ds(at, chunk), later] = ref[pl.ds(pl.multiple_of(start + LAG, LAG), chunk), :] * mask
            if with_mask:
                out_ref[pl.ds(at, chunk), pl.ds(512, 128)] = mask
            return carry

        lax.fori_loop(0, middle // chunk, body, 0)


def spread(first, second, mask, with_mask):
    middle, width = mask.shape[0] // 2, 640 if with_mask else 512
    out = jax.ShapeDtypeStruct((middle, width), jnp.bfloat16)
    vmem = pl.BlockSpec(memory_space=pltpu.VMEM)
    return pl.pallas_call(
        functools.partial(spread_kernel, with_mask),
        out_shape=(out, out),
        in_specs=[vmem] * 3,
        out_specs=(vmem, vmem),
        compiler_params=pltpu.CompilerParams(vmem_limit_bytes=16 << 20),
    )(first, second, mask)


def finish_kernel(bit0_ref, a_ref, b_ref, c_ref, d_ref, zero_ref, lag_ref):
    total = a_ref[...] + b_ref[...] + c_ref[...] + d_ref[...]
    count = total[LAG + 3 : LAG + 4, :1]
    cols, lags, line = (total[LAG + i : LAG + i + 1] / count for i in range(3))
    row = lax.broadcasted_iota(jnp.int32, (LAG, 128), 0) + bit0_ref[0] * LAG
    lane = lax.broadcasted_iota(jnp.int32, (LAG, 128), 1)
    means = jnp.sum(jnp.where(lane == row, jnp.broadcast_to(line, (LAG, 128)), 0.0), axis=1, keepdims=True)
    zero_ref[...] = total[:LAG] / count - means * cols
    lag_ref[...] = total[LAG + 8 :] / count - means * lags


def finish(bit0, parts):
    out = jax.ShapeDtypeStruct((LAG, 128), jnp.float32)
    vmem = pl.BlockSpec(memory_space=pltpu.VMEM)
    return pl.pallas_call(
        finish_kernel,
        out_shape=(out, out),
        in_specs=[pl.BlockSpec(memory_space=pltpu.SMEM)] + [vmem] * 4,
        out_specs=(vmem, vmem),
        name="finish",
        compiler_params=pltpu.CompilerParams(vmem_limit_bytes=4 << 20),
    )(bit0.reshape(1).astype(jnp.int32), *parts)


def shards(frames_data, traj_ids):
    frame, block = lax.axis_index("frames"), lax.axis_index("blocks")
    x_lo, z = frame // 16, frame % 16
    x_hi, y, core = block // 8, (block // 2) % 4, block % 2
    z_high, bit1, bit0 = z // 4, (z // 2) % 2, z % 2
    same_x, same_c = x_lo == x_hi, bit1 == core

    own = frames_data
    rows = own.shape[0]
    middle = rows // 2
    up, down = send(own, up_y), send(own, down_y)
    x_body = send(own, swap_x_hi)
    marks = traj_ids + 1
    mark_rows = jnp.pad(marks[None, :LAG].astype(jnp.bfloat16), ((0, 15), (0, 128 - LAG)))
    tip = send(jnp.concatenate([own[:LAG], mark_rows]), to_previous)
    own_ext = jnp.concatenate([own, tip[:LAG]])
    over_core = send(own_ext, swap_core)
    over_x = jnp.concatenate([x_body, send(tip[:LAG], swap_x_hi)])
    far_a = send(up[:middle], up_y)
    far_b = send(down[middle:], down_y)
    over_both = send(over_x, swap_core)

    rim = tip[LAG, :LAG].astype(jnp.int32)
    valid = jnp.concatenate([marks[LAG:], rim]) == marks
    count_here = jnp.sum(valid.astype(jnp.float32))
    mask = lax.optimization_barrier(jnp.broadcast_to(valid.astype(jnp.bfloat16)[:, None], (rows, 128)))

    near_cols = spread(own_ext, over_core, mask, True)
    over_cols = spread(over_x, over_both, mask, False)
    ones = jnp.ones((middle, 8), jnp.bfloat16)
    left = [
        lax.optimization_barrier(jnp.concatenate([own[part], down[part], up[part], ones], axis=1))
        for part in (slice(0, middle), slice(middle, rows))
    ]
    beyond = (far_a, far_b)

    def product(lefts, rights):
        return contract(lefts[0], rights[0]) + contract(lefts[1], rights[1])

    side_near, side_over = product(left, near_cols), product(left, over_cols)
    far_near, far_over = product(beyond, near_cols), product(beyond, over_cols)
    sums_side = contract(mask[:middle, :8], left[0])[0] + contract(mask[middle:, :8], left[1])[0]
    sums_far = jnp.sum(jnp.where(jnp.eye(128, dtype=bool), far_near[:, 512:], 0.0), axis=0)
    sums_left = jnp.concatenate([sums_side[:384], sums_far]).reshape(4, 1, 128)

    def tiles(side, far, first):
        return jnp.concatenate([side[:384, first : first + 256], far[:, first : first + 256]]).reshape(4, 2, LAG, 256)

    def with_sums(tile, side):
        extra = jnp.concatenate(
            [
                jnp.broadcast_to(side[384, :256], (4, 1, 256)),
                jnp.broadcast_to(side[384, 256:512], (4, 1, 256)),
                jnp.tile(sums_left, (1, 1, 2)),
                jnp.broadcast_to(count_here, (4, 5, 256)),
            ],
            axis=1,
        )
        return jnp.concatenate([tile, jnp.broadcast_to(extra[:, None], (4, 2, 8, 256))], axis=2)

    plain_near = with_sums(tiles(side_near, far_near, 0), side_near)
    plain_over = with_sums(tiles(side_over, far_over, 0), side_over)
    lagged = jnp.concatenate([tiles(side_near, far_near, 256), tiles(side_over, far_over, 256)], axis=3)

    def by_x(near_part, over_part):
        return jnp.where(same_x, near_part, over_part), jnp.where(same_x, over_part, near_part)

    def by_core(value):
        return jnp.where(same_c, value[..., :128], value[..., 128:]), jnp.where(same_c, value[..., 128:], value[..., :128])

    def by_half(value):
        return (
            lax.dynamic_index_in_dim(value, bit0, 1, keepdims=False),
            lax.dynamic_index_in_dim(value, 1 - bit0, 1, keepdims=False),
        )

    def step(halves, move):
        kept, sent = halves
        return kept + send(sent, move)

    plain = step(by_x(plain_near, plain_over), swap_x_lo)
    lagged = step(by_half(lagged), near_shifted(1))
    plain = step(by_half(plain), near(1))
    lagged = step(by_x(lagged[..., :256], lagged[..., 256:]), swap_x_lo)
    plain = step(by_core(plain), near(2))
    lagged = step(by_core(lagged), near_shifted(2))
    pieces = jnp.concatenate([plain, lagged], axis=1)

    parts = []
    for move in (2, 1, 3, 0):
        away = (z_high + move - y) % 4
        piece = lax.dynamic_index_in_dim(pieces, away ^ (away // 2), 0, keepdims=False)
        parts.append(send(piece, to_owner(move)))
    return finish(bit0, parts)


def solution(mesh):
    return jax.shard_map(
        shards,
        mesh=mesh,
        in_specs=(P("frames", "blocks"), P("frames")),
        out_specs=(P("frames", "blocks"), P("frames", "blocks")),
        check_vma=False,
    )
```

```python
import functools

import jax
import jax.numpy as jnp
from jax import lax
from jax.experimental import pallas as pl
from jax.experimental.pallas import tpu as pltpu
from jax.sharding import PartitionSpec as P


LAG = 64
AXES = ("frames", "blocks")


def pairs(move):
    out = []
    for frame in range(32):
        for block in range(16):
            target = move(frame // 16, frame % 16, block // 8, (block // 2) % 4, block % 2)
            if target is None:
                continue
            xl, z, xh, y, c = target
            out.append((frame * 16 + block, (xl * 16 + z % 16) * 16 + xh * 8 + (y % 4) * 2 + c))
    return out


def send(value, move):
    return lax.ppermute(value, AXES, pairs(move))


def to_previous(xl, z, xh, y, c):
    frame = xl * 16 + z - 1
    return None if frame < 0 else (frame // 16, frame % 16, xh, y, c)


def up_y(xl, z, xh, y, c):
    return (xl, z, xh, y + 1, c)


def down_y(xl, z, xh, y, c):
    return (xl, z, xh, y - 1, c)


def swap_x_hi(xl, z, xh, y, c):
    return (xl, z, 1 - xh, y, c)


def swap_core(xl, z, xh, y, c):
    return (xl, z, xh, y, 1 - c)


def swap_x_lo(xl, z, xh, y, c):
    return (1 - xl, z, xh, y, c)


def near(step):
    return lambda xl, z, xh, y, c: (xl, z ^ step, xh, y, c)


def near_shifted(step):
    return lambda xl, z, xh, y, c: (xl, z + step if z & step else z - step, xh, y, c)


def to_owner(step):
    def move(xl, z, xh, y, c):
        high, bit1, bit0 = (z // 4 + step) % 4, (z // 2) % 2, z % 2
        return (xh, high * 4 + c * 2 + bit0, xl, y, bit1)

    return move


def contract(left, right):
    return lax.dot_general(left, right, (((0,), (0,)), ((), ())), preferred_element_type=jnp.float32)


def spread_kernel(with_mask, first_ref, second_ref, mask_ref, out_ref):
    chunk = 256

    def body(i, carry):
        start = pl.multiple_of(i * chunk, chunk)
        ahead = pl.multiple_of(start + LAG, LAG)
        mask = mask_ref[pl.ds(start, chunk), :]
        for column, ref in enumerate((first_ref, second_ref)):
            now, later = pl.ds(column * 128, 128), pl.ds(256 + column * 128, 128)
            out_ref[pl.ds(start, chunk), now] = ref[pl.ds(start, chunk), :] * mask
            out_ref[pl.ds(start, chunk), later] = ref[pl.ds(ahead, chunk), :] * mask
        if with_mask:
            out_ref[pl.ds(start, chunk), pl.ds(512, 128)] = mask
        return carry

    lax.fori_loop(0, out_ref.shape[0] // chunk, body, 0)


def spread(first, second, mask, with_mask):
    vmem = pl.BlockSpec(memory_space=pltpu.VMEM)
    return pl.pallas_call(
        functools.partial(spread_kernel, with_mask),
        out_shape=jax.ShapeDtypeStruct((mask.shape[0], 640 if with_mask else 512), jnp.bfloat16),
        in_specs=[vmem] * 3,
        out_specs=vmem,
        compiler_params=pltpu.CompilerParams(vmem_limit_bytes=16 << 20),
    )(first, second, mask)


def finish_kernel(bit0_ref, a_ref, b_ref, c_ref, d_ref, zero_ref, lag_ref):
    total = a_ref[...] + b_ref[...] + c_ref[...] + d_ref[...]
    count = total[LAG + 3 : LAG + 4, :1]
    cols, lags, line = (total[LAG + i : LAG + i + 1] / count for i in range(3))
    row = lax.broadcasted_iota(jnp.int32, (LAG, 128), 0) + bit0_ref[0] * LAG
    lane = lax.broadcasted_iota(jnp.int32, (LAG, 128), 1)
    means = jnp.sum(jnp.where(lane == row, jnp.broadcast_to(line, (LAG, 128)), 0.0), axis=1, keepdims=True)
    zero_ref[...] = total[:LAG] / count - means * cols
    lag_ref[...] = total[LAG + 8 :] / count - means * lags


def finish(bit0, parts):
    out = jax.ShapeDtypeStruct((LAG, 128), jnp.float32)
    vmem = pl.BlockSpec(memory_space=pltpu.VMEM)
    return pl.pallas_call(
        finish_kernel,
        out_shape=(out, out),
        in_specs=[pl.BlockSpec(memory_space=pltpu.SMEM)] + [vmem] * 4,
        out_specs=(vmem, vmem),
        name="finish",
        compiler_params=pltpu.CompilerParams(vmem_limit_bytes=4 << 20),
    )(bit0.reshape(1).astype(jnp.int32), *parts)


def shards(frames_data, traj_ids):
    frame, block = lax.axis_index("frames"), lax.axis_index("blocks")
    x_lo, z = frame // 16, frame % 16
    x_hi, y, core = block // 8, (block // 2) % 4, block % 2
    z_high, bit1, bit0 = z // 4, (z // 2) % 2, z % 2
    same_x, same_c = x_lo == x_hi, bit1 == core

    own = frames_data
    rows = own.shape[0]
    middle = rows // 2
    up, down = send(own, up_y), send(own, down_y)
    x_body = send(own, swap_x_hi)
    marks = traj_ids + 1
    mark_rows = jnp.pad(marks[None, :LAG].astype(jnp.bfloat16), ((0, 15), (0, 128 - LAG)))
    tip = send(jnp.concatenate([own[:LAG], mark_rows]), to_previous)
    own_ext = jnp.concatenate([own, tip[:LAG]])
    over_core = send(own_ext, swap_core)
    over_x = jnp.concatenate([x_body, send(tip[:LAG], swap_x_hi)])
    far_a = send(up[:middle], up_y)
    far_b = send(down[middle:], down_y)
    over_both = send(over_x, swap_core)

    rim = tip[LAG, :LAG].astype(jnp.int32)
    valid = jnp.concatenate([marks[LAG:], rim]) == marks
    mask = lax.optimization_barrier(jnp.broadcast_to(valid.astype(jnp.bfloat16)[:, None], (rows, 128)))

    near_cols = spread(own_ext, over_core, mask, True)
    over_cols = spread(over_x, over_both, mask, False)
    ones = jnp.ones((rows, 8), jnp.bfloat16)
    left = lax.optimization_barrier(jnp.concatenate([own, down, up, ones], axis=1))

    beyond = jnp.concatenate([far_a, far_b])
    side_near, side_over = contract(left, near_cols), contract(left, over_cols)
    far_near, far_over = contract(beyond, near_cols), contract(beyond, over_cols)
    eye = jnp.eye(128, dtype=bool)

    def with_sums(plain, sums, side):
        groups = plain.shape[0] // 128
        line_count = jnp.tile(side_near[384, 512:], 2)
        extra = jnp.concatenate(
            [
                jnp.broadcast_to(side[384, :256], (groups, 1, 256)),
                jnp.broadcast_to(side[384, 256:512], (groups, 1, 256)),
                jnp.tile(sums[:, None], (1, 1, 2)),
                jnp.broadcast_to(line_count, (groups, 5, 256)),
            ],
            axis=1,
        )
        extra = jnp.broadcast_to(extra[:, None], (groups, 2, 8, 256))
        return jnp.concatenate([plain.reshape(groups, 2, LAG, 256), extra], axis=2)

    def split(near, over):
        groups = near.shape[0] // 128
        sums = jnp.sum(jnp.where(eye, near[:, 512:].reshape(groups, 128, 128), 0.0), axis=1)
        plain = (with_sums(near[:, :256], sums, side_near), with_sums(over[:, :256], sums, side_over))
        lagged = jnp.concatenate([near[:, 256:512], over[:, 256:]], axis=1).reshape(groups, 2, LAG, 512)
        return plain, lagged

    side_plain, side_lagged = split(side_near[:384], side_over[:384])
    far_plain, far_lagged = split(far_near, far_over)

    def by_x(near_part, over_part):
        return jnp.where(same_x, near_part, over_part), jnp.where(same_x, over_part, near_part)

    def by_core(value):
        return jnp.where(same_c, value[..., :128], value[..., 128:]), jnp.where(same_c, value[..., 128:], value[..., :128])

    def by_half(value):
        return (
            lax.dynamic_index_in_dim(value, bit0, 1, keepdims=False),
            lax.dynamic_index_in_dim(value, 1 - bit0, 1, keepdims=False),
        )

    def step(halves, move):
        kept, sent = halves
        return kept + send(sent, move)

    plain_a = step(by_x(*side_plain), swap_x_lo)
    lagged_a = step(by_half(side_lagged), near(1))
    plain_b = step(by_x(*far_plain), swap_x_lo)
    lagged_b = step(by_half(far_lagged), near(1))
    plain, lagged = jnp.concatenate([plain_a, plain_b]), jnp.concatenate([lagged_a, lagged_b])
    plain = step(by_half(plain), near(1))
    lagged = step(by_x(lagged[..., :256], lagged[..., 256:]), swap_x_lo)
    plain = step(by_core(plain), near(2))
    lagged = step(by_core(lagged), near_shifted(2))
    pieces = jnp.concatenate([plain, lagged], axis=1)

    parts = []
    for move in (2, 1, 3, 0):
        away = (z_high + move - y) % 4
        piece = lax.dynamic_index_in_dim(pieces, away ^ (away // 2), 0, keepdims=False)
        parts.append(send(piece, to_owner(move)))
    return finish(bit0, parts)


def solution(mesh):
    return jax.shard_map(
        shards,
        mesh=mesh,
        in_specs=(P("frames", "blocks"), P("frames")),
        out_specs=(P("frames", "blocks"), P("frames", "blocks")),
        check_vma=False,
    )
```

```python
import functools

import jax
import jax.numpy as jnp
from jax import lax
from jax.experimental import pallas as pl
from jax.experimental.pallas import tpu as pltpu
from jax.sharding import PartitionSpec as P


LAG = 64
AXES = ("frames", "blocks")
VMEM = pl.BlockSpec(memory_space=pltpu.VMEM)
SMEM = pl.BlockSpec(memory_space=pltpu.SMEM)


def pairs(move):
    out = []
    for frame in range(32):
        for block in range(16):
            target = move(frame // 16, frame % 16, block // 8, (block // 2) % 4, block % 2)
            if target is None:
                continue
            xl, z, xh, y, c = target
            out.append((frame * 16 + block, (xl * 16 + z % 16) * 16 + xh * 8 + (y % 4) * 2 + c))
    return out


def send(value, move):
    return lax.ppermute(value, AXES, pairs(move))


def to_previous(xl, z, xh, y, c):
    frame = xl * 16 + z - 1
    return None if frame < 0 else (frame // 16, frame % 16, xh, y, c)


def up_y(xl, z, xh, y, c):
    return (xl, z, xh, y + 1, c)


def down_y(xl, z, xh, y, c):
    return (xl, z, xh, y - 1, c)


def swap_x_hi(xl, z, xh, y, c):
    return (xl, z, 1 - xh, y, c)


def swap_core(xl, z, xh, y, c):
    return (xl, z, xh, y, 1 - c)


def swap_x_lo(xl, z, xh, y, c):
    return (1 - xl, z, xh, y, c)


def near(step):
    return lambda xl, z, xh, y, c: (xl, z ^ step, xh, y, c)


def near_shifted(step):
    return lambda xl, z, xh, y, c: (xl, z + step if z & step else z - step, xh, y, c)


def to_owner(step):
    def move(xl, z, xh, y, c):
        high, bit1, bit0 = (z // 4 + step) % 4, (z // 2) % 2, z % 2
        return (xh, high * 4 + c * 2 + bit0, xl, y, bit1)

    return move


def contract(left, right):
    return lax.dot_general(left, right, (((0,), (0,)), ((), ())), preferred_element_type=jnp.float32)


def spread_kernel(with_mask, first_ref, second_ref, tips_ref, mask_ref, out_ref):
    chunk, bodies = 256, (first_ref, second_ref)
    last = out_ref.shape[0] - chunk

    def store(count, lane, value, at):
        out_ref[pl.ds(at, count), pl.ds(lane, 128)] = value * mask_ref[pl.ds(at, count), :]

    def now_columns(start):
        for column, ref in enumerate(bodies):
            store(chunk, column * 128, ref[pl.ds(start, chunk), :], start)
        if with_mask:
            out_ref[pl.ds(start, chunk), pl.ds(512, 128)] = mask_ref[pl.ds(start, chunk), :]

    def body(i, carry):
        start = pl.multiple_of(i * chunk, chunk)
        ahead = pl.multiple_of(start + LAG, LAG)
        now_columns(start)
        for column, ref in enumerate(bodies):
            store(chunk, 256 + column * 128, ref[pl.ds(ahead, chunk), :], start)
        return carry

    lax.fori_loop(0, last // chunk, body, 0)
    now_columns(last)
    for column, ref in enumerate(bodies):
        lane = 256 + column * 128
        store(chunk - LAG, lane, ref[last + LAG :, :], last)
        store(LAG, lane, tips_ref[column * LAG : (column + 1) * LAG, :], last + chunk - LAG)


def spread(first, second, tips, mask, with_mask):
    return pl.pallas_call(
        functools.partial(spread_kernel, with_mask),
        out_shape=jax.ShapeDtypeStruct((mask.shape[0], 640 if with_mask else 512), jnp.bfloat16),
        in_specs=[VMEM] * 4,
        out_specs=VMEM,
        compiler_params=pltpu.CompilerParams(vmem_limit_bytes=9 << 20),
    )(first, second, tips, mask)


def local_call(kernel, shapes, flags, *args):
    return pl.pallas_call(
        kernel,
        out_shape=tuple(jax.ShapeDtypeStruct(shape, jnp.float32) for shape in shapes),
        in_specs=[SMEM] + [VMEM] * len(args),
        out_specs=(VMEM,) * len(shapes),
        compiler_params=pltpu.CompilerParams(vmem_limit_bytes=9 << 20),
    )(flags, *args)


def arrange_kernel(groups, flags, near, over, line_near, line_over, plain_keep, plain_send, lag_keep, lag_send):
    keep_near, half = flags[0] == 1, flags[1]
    eye = lax.broadcasted_iota(jnp.int32, (128, 128), 0) == lax.broadcasted_iota(jnp.int32, (128, 128), 1)
    row = lax.broadcasted_iota(jnp.int32, (8, 256), 0)

    def wide(value):
        return jnp.broadcast_to(value, (8, value.shape[1]))

    count = wide(jnp.concatenate([line_near[384:385, 512:]] * 2, axis=1))
    lines = [[wide(ref[384:385, at : at + 256]) for at in (0, 256)] for ref in (line_near, line_over)]
    for group in range(groups):
        rows = slice(group * 128, group * 128 + 128)
        sums = jnp.sum(jnp.where(eye, near[rows, 512:], 0.0), axis=0, keepdims=True)
        sums = wide(jnp.concatenate([sums, sums], axis=1))
        for out, take_near in ((plain_keep, keep_near), (plain_send, jnp.logical_not(keep_near))):
            out[group, :128, :] = jnp.where(take_near, near[rows, :256], over[rows, :256])
            now, later = (jnp.where(take_near, a, b) for a, b in zip(*lines))
            out[group, 128:, :] = jnp.where(row == 0, now, jnp.where(row == 1, later, jnp.where(row == 2, sums, count)))
        for out, index in ((lag_keep, half), (lag_send, 1 - half)):
            part = pl.ds(pl.multiple_of(group * 128 + index * LAG, LAG), LAG)
            out[group, :, :256] = near[part, 256:512]
            out[group, :, 256:] = over[part, 256:512]


def arrange(flags, near, over, line_near, line_over, groups):
    shapes = [(groups, 136, 256)] * 2 + [(groups, LAG, 512)] * 2
    return local_call(functools.partial(arrange_kernel, groups), shapes, flags, near, over, line_near, line_over)


def merge_plain_kernel(flags, keep_a, got_a, keep_b, got_b, keep, send_out):
    for out, index in ((keep, flags[1]), (send_out, 1 - flags[1])):
        part = pl.ds(pl.multiple_of(index * LAG, LAG), LAG)
        for at, mine, got in ((0, keep_a, got_a), (3, keep_b, got_b)):
            for group in range(mine.shape[0]):
                out[at + group, :LAG, :] = mine[group, part, :] + got[group, part, :]
                out[at + group, LAG:, :] = mine[group, 128:, :] + got[group, 128:, :]


def merge_lag_kernel(flags, keep_a, got_a, keep_b, got_b, keep, send_out):
    keep_near = flags[0] == 1
    for at, mine, got in ((0, keep_a, got_a), (3, keep_b, got_b)):
        for group in range(mine.shape[0]):
            near_part = mine[group, :, :256] + got[group, :, :256]
            over_part = mine[group, :, 256:] + got[group, :, 256:]
            keep[at + group] = jnp.where(keep_near, near_part, over_part)
            send_out[at + group] = jnp.where(keep_near, over_part, near_part)


def finish_kernel(flags, a_ref, b_ref, c_ref, d_ref, zero_ref, lag_ref):
    total = a_ref[...] + b_ref[...] + c_ref[...] + d_ref[...]
    count = total[LAG + 3 : LAG + 4, :1]
    cols, lags, line = (total[LAG + i : LAG + i + 1] / count for i in range(3))
    row = lax.broadcasted_iota(jnp.int32, (LAG, 128), 0) + flags[1] * LAG
    lane = lax.broadcasted_iota(jnp.int32, (LAG, 128), 1)
    means = jnp.sum(jnp.where(lane == row, jnp.broadcast_to(line, (LAG, 128)), 0.0), axis=1, keepdims=True)
    zero_ref[...] = total[:LAG] / count - means * cols
    lag_ref[...] = total[LAG + 8 :] / count - means * lags


def finish(flags, parts):
    return local_call(finish_kernel, [(LAG, 128)] * 2, flags, *parts)


def shards(frames_data, traj_ids):
    frame, block = lax.axis_index("frames"), lax.axis_index("blocks")
    x_lo, z = frame // 16, frame % 16
    x_hi, y, core = block // 8, (block // 2) % 4, block % 2
    z_high, bit1, bit0 = z // 4, (z // 2) % 2, z % 2
    same_x, same_c = x_lo == x_hi, bit1 == core

    own = frames_data
    rows = own.shape[0]
    middle = rows // 2
    up, down = send(own, up_y), send(own, down_y)
    over_x = send(own, swap_x_hi)
    over_core = send(own, swap_core)
    marks = traj_ids + 1
    mark_rows = jnp.pad(marks[None, :LAG].astype(jnp.bfloat16), ((0, 15), (0, 128 - LAG)))
    tip = send(jnp.concatenate([own[:LAG], over_core[:LAG], mark_rows]), to_previous)
    near_tips = tip[: 2 * LAG]
    over_tips = send(near_tips, swap_x_hi)
    up_part, down_part = up[:middle], down[middle:]
    far_a, far_b = send(up_part, up_y), send(down_part, down_y)
    over_both = send(over_x, swap_core)

    rim = tip[2 * LAG, :LAG].astype(jnp.int32)
    valid = jnp.concatenate([marks[LAG:], rim]) == marks
    mask = lax.optimization_barrier(jnp.broadcast_to(valid.astype(jnp.bfloat16)[:, None], (rows, 128)))

    near_cols = spread(own, over_core, near_tips, mask, True)
    over_cols = spread(over_x, over_both, over_tips, mask, False)
    ones = jnp.ones((rows, 8), jnp.bfloat16)
    left = lax.optimization_barrier(jnp.concatenate([own, down, up, ones], axis=1))

    beyond = jnp.concatenate([far_a, far_b])
    side_near, side_over = contract(left, near_cols), contract(left, over_cols)
    far_near, far_over = contract(beyond, near_cols), contract(beyond, over_cols)
    flags = jnp.stack([same_x.astype(jnp.int32), bit0.astype(jnp.int32)])
    side = arrange(flags, side_near, side_over, side_near, side_over, 3)
    far = arrange(flags, far_near, far_over, side_near, side_over, 1)
    plain_a, lagged_a = send(side[1], swap_x_lo), send(side[3], near(1))
    plain_b, lagged_b = send(far[1], swap_x_lo), send(far[3], near(1))

    kept, sent = local_call(merge_lag_kernel, [(4, LAG, 256)] * 2, flags, side[2], lagged_a, far[2], lagged_b)
    lagged = kept + send(sent, swap_x_lo)
    kept, sent = local_call(merge_plain_kernel, [(4, 72, 256)] * 2, flags, side[0], plain_a, far[0], plain_b)
    plain = kept + send(sent, near(1))

    def by_core(value):
        return jnp.where(same_c, value[..., :128], value[..., 128:]), jnp.where(same_c, value[..., 128:], value[..., :128])

    kept, sent = by_core(plain)
    plain = kept + send(sent, near(2))
    kept, sent = by_core(lagged)
    lagged = kept + send(sent, near_shifted(2))
    pieces = jnp.concatenate([plain, lagged], axis=1)

    parts = []
    for move in (2, 1, 3, 0):
        away = (z_high + move - y) % 4
        piece = lax.dynamic_index_in_dim(pieces, away ^ (away // 2), 0, keepdims=False)
        parts.append(send(piece, to_owner(move)))
    return finish(flags, parts)


def solution(mesh):
    return jax.shard_map(
        shards,
        mesh=mesh,
        in_specs=(P("frames", "blocks"), P("frames")),
        out_specs=(P("frames", "blocks"), P("frames", "blocks")),
        check_vma=False,
    )
```

```python
import functools

import jax
import jax.numpy as jnp
from jax import lax
from jax.experimental import pallas as pl
from jax.experimental.pallas import tpu as pltpu
from jax.sharding import PartitionSpec as P


LAG = 64
AXES = ("frames", "blocks")
VMEM = pl.BlockSpec(memory_space=pltpu.VMEM)


def pairs(move):
    out = []
    for frame in range(32):
        for block in range(16):
            target = move(frame // 16, frame % 16, block // 8, (block // 2) % 4, block % 2)
            if target is None:
                continue
            xl, z, xh, y, c = target
            out.append((frame * 16 + block, (xl * 16 + z % 16) * 16 + xh * 8 + (y % 4) * 2 + c))
    return out


def send(value, move):
    return lax.ppermute(value, AXES, pairs(move))


def to_previous(xl, z, xh, y, c):
    frame = xl * 16 + z - 1
    return None if frame < 0 else (frame // 16, frame % 16, xh, y, c)


def up_y(xl, z, xh, y, c):
    return (xl, z, xh, y + 1, c)


def down_y(xl, z, xh, y, c):
    return (xl, z, xh, y - 1, c)


def swap_x_hi(xl, z, xh, y, c):
    return (xl, z, 1 - xh, y, c)


def swap_core(xl, z, xh, y, c):
    return (xl, z, xh, y, 1 - c)


def swap_x_lo(xl, z, xh, y, c):
    return (1 - xl, z, xh, y, c)


def near(step):
    return lambda xl, z, xh, y, c: (xl, z ^ step, xh, y, c)


def near_shifted(step):
    return lambda xl, z, xh, y, c: (xl, z + step if z & step else z - step, xh, y, c)


def to_owner(step):
    def move(xl, z, xh, y, c):
        high, bit1, bit0 = (z // 4 + step) % 4, (z // 2) % 2, z % 2
        return (xh, high * 4 + c * 2 + bit0, xl, y, bit1)

    return move


def contract(left, right):
    return lax.dot_general(left, right, (((0,), (0,)), ((), ())), preferred_element_type=jnp.float32)


def spread_kernel(with_mask, first_ref, second_ref, tips_ref, mask_ref, out_ref):
    chunk, bodies = 256, (first_ref, second_ref)
    last = out_ref.shape[0] - chunk

    def store(count, lane, value, at):
        out_ref[pl.ds(at, count), pl.ds(lane, 128)] = value * mask_ref[pl.ds(at, count), :]

    def now_columns(start):
        for column, ref in enumerate(bodies):
            store(chunk, column * 128, ref[pl.ds(start, chunk), :], start)
        if with_mask:
            out_ref[pl.ds(start, chunk), pl.ds(512, 128)] = mask_ref[pl.ds(start, chunk), :]

    def body(i, carry):
        start = pl.multiple_of(i * chunk, chunk)
        ahead = pl.multiple_of(start + LAG, LAG)
        now_columns(start)
        for column, ref in enumerate(bodies):
            store(chunk, 256 + column * 128, ref[pl.ds(ahead, chunk), :], start)
        return carry

    lax.fori_loop(0, last // chunk, body, 0)
    now_columns(last)
    for column, ref in enumerate(bodies):
        lane = 256 + column * 128
        store(chunk - LAG, lane, ref[last + LAG :, :], last)
        store(LAG, lane, tips_ref[column * LAG : (column + 1) * LAG, :], last + chunk - LAG)


def spread(first, second, tips, mask, with_mask):
    return pl.pallas_call(
        functools.partial(spread_kernel, with_mask),
        out_shape=jax.ShapeDtypeStruct((mask.shape[0], 640 if with_mask else 512), jnp.bfloat16),
        in_specs=[VMEM] * 4,
        out_specs=VMEM,
        compiler_params=pltpu.CompilerParams(vmem_limit_bytes=9 << 20),
    )(first, second, tips, mask)


def local_call(kernel, shapes, *args):
    return pl.pallas_call(
        kernel,
        out_shape=tuple(jax.ShapeDtypeStruct(shape, jnp.float32) for shape in shapes),
        in_specs=[VMEM] * len(args),
        out_specs=(VMEM,) * len(shapes),
        compiler_params=pltpu.CompilerParams(vmem_limit_bytes=9 << 20),
    )(*args)


def position():
    frame, block = lax.axis_index("frames"), lax.axis_index("blocks")
    return frame >> 4, frame & 15, block >> 3, (block >> 1) & 3, block & 1


def kept_x():
    x_lo, _, x_hi, _, _ = position()
    return x_lo == x_hi


def low_bit():
    return position()[1] & 1


def arrange_kernel(groups, *refs):
    nears, overs, refs = refs[:groups], refs[groups : 2 * groups], refs[2 * groups :]
    line_near, line_over, plain_keep, plain_send, lag_keep, lag_send = refs
    keep_near, half = kept_x(), low_bit()
    eye = lax.broadcasted_iota(jnp.int32, (128, 128), 0) == lax.broadcasted_iota(jnp.int32, (128, 128), 1)
    row = lax.broadcasted_iota(jnp.int32, (8, 256), 0)

    def wide(value):
        return jnp.broadcast_to(value, (8, value.shape[1]))

    count = wide(jnp.concatenate([line_near[128:129, 512:]] * 2, axis=1))
    lines = [[wide(ref[128:129, at : at + 256]) for at in (0, 256)] for ref in (line_near, line_over)]
    for group, (near_ref, over_ref) in enumerate(zip(nears, overs)):
        sums = jnp.sum(jnp.where(eye, near_ref[:128, 512:], 0.0), axis=0, keepdims=True)
        sums = wide(jnp.concatenate([sums, sums], axis=1))
        for out, take_near in ((plain_keep, keep_near), (plain_send, jnp.logical_not(keep_near))):
            out[group, :128, :] = jnp.where(take_near, near_ref[:128, :256], over_ref[:128, :256])
            now, later = (jnp.where(take_near, a, b) for a, b in zip(*lines))
            out[group, 128:, :] = jnp.where(row == 0, now, jnp.where(row == 1, later, jnp.where(row == 2, sums, count)))
        for out, index in ((lag_keep, half), (lag_send, 1 - half)):
            part = pl.ds(pl.multiple_of(index * LAG, LAG), LAG)
            out[group, :, :256] = near_ref[part, 256:512]
            out[group, :, 256:] = over_ref[part, 256:512]


def arrange(nears, overs, lines):
    groups = len(nears)
    shapes = [(groups, 136, 256)] * 2 + [(groups, LAG, 512)] * 2
    return local_call(functools.partial(arrange_kernel, groups), shapes, *nears, *overs, *lines)


def split_core_kernel(mine, got, keep, send_out):
    _, z, _, _, core = position()
    same = ((z >> 1) & 1) == core
    total = mine[...] + got[...]
    low, high = total[:, :, :128], total[:, :, 128:]
    keep[...] = jnp.where(same, low, high)
    send_out[...] = jnp.where(same, high, low)


def merge_plain_kernel(keep_a, got_a, keep_b, got_b, keep, send_out):
    for out, index in ((keep, low_bit()), (send_out, 1 - low_bit())):
        part = pl.ds(pl.multiple_of(index * LAG, LAG), LAG)
        for at, mine, got in ((0, keep_a, got_a), (3, keep_b, got_b)):
            for group in range(mine.shape[0]):
                out[at + group, :LAG, :] = mine[group, part, :] + got[group, part, :]
                out[at + group, LAG:, :] = mine[group, 128:, :] + got[group, 128:, :]


def merge_lag_kernel(keep_a, got_a, keep_b, got_b, keep, send_out):
    keep_near = kept_x()
    for at, mine, got in ((0, keep_a, got_a), (3, keep_b, got_b)):
        for group in range(mine.shape[0]):
            near_part = mine[group, :, :256] + got[group, :, :256]
            over_part = mine[group, :, 256:] + got[group, :, 256:]
            keep[at + group] = jnp.where(keep_near, near_part, over_part)
            send_out[at + group] = jnp.where(keep_near, over_part, near_part)


def finish_kernel(a_ref, b_ref, c_ref, d_ref, zero_ref, lag_ref):
    total = a_ref[...] + b_ref[...] + c_ref[...] + d_ref[...]
    count = total[LAG + 3 : LAG + 4, :1]
    cols, lags, line = (total[LAG + i : LAG + i + 1] / count for i in range(3))
    row = lax.broadcasted_iota(jnp.int32, (LAG, 128), 0) + low_bit() * LAG
    lane = lax.broadcasted_iota(jnp.int32, (LAG, 128), 1)
    means = jnp.sum(jnp.where(lane == row, jnp.broadcast_to(line, (LAG, 128)), 0.0), axis=1, keepdims=True)
    zero_ref[...] = total[:LAG] / count - means * cols
    lag_ref[...] = total[LAG + 8 :] / count - means * lags


def finish(parts):
    return local_call(finish_kernel, [(LAG, 128)] * 2, *parts)


def shards(frames_data, traj_ids):
    _, z, _, y, _ = position()
    z_high = z >> 2

    own = frames_data
    rows = own.shape[0]
    middle = rows // 2
    up, down = send(own, up_y), send(own, down_y)
    over_x = send(own, swap_x_hi)
    over_core = send(own, swap_core)
    marks = traj_ids + 1
    mark_rows = jnp.pad(marks[None, :LAG].astype(jnp.bfloat16), ((0, 15), (0, 128 - LAG)))
    tip = send(jnp.concatenate([own[:LAG], over_core[:LAG], mark_rows]), to_previous)
    near_tips = tip[: 2 * LAG]
    over_tips = send(near_tips, swap_x_hi)
    up_part, down_part = up[:middle], down[middle:]
    far_a, far_b = send(up_part, up_y), send(down_part, down_y)
    over_both = send(over_x, swap_core)

    rim = tip[2 * LAG, :LAG].astype(jnp.int32)
    valid = jnp.concatenate([marks[LAG:], rim]) == marks
    mask = lax.optimization_barrier(jnp.broadcast_to(valid.astype(jnp.bfloat16)[:, None], (rows, 128)))

    near_cols = spread(own, over_core, near_tips, mask, True)
    over_cols = spread(over_x, over_both, over_tips, mask, False)
    own_ones = lax.optimization_barrier(jnp.concatenate([own, jnp.ones((rows, 8), jnp.bfloat16)], axis=1))

    sides = (own_ones, down, up)
    side_near = [contract(left, near_cols) for left in sides]
    side_over = [contract(left, over_cols) for left in sides]
    beyond = jnp.concatenate([far_a, far_b])
    far_near, far_over = contract(beyond, near_cols), contract(beyond, over_cols)

    lines = (side_near[0], side_over[0])
    side = arrange(side_near, side_over, lines)
    far = arrange([far_near], [far_over], lines)
    plain_a, lagged_a = send(side[1], swap_x_lo), send(side[3], near(1))
    plain_b, lagged_b = send(far[1], swap_x_lo), send(far[3], near(1))

    def local(kernel, count, columns, *args):
        return local_call(kernel, [(4, count, columns)] * 2, *args)

    kept, sent = local(merge_plain_kernel, 72, 256, side[0], plain_a, far[0], plain_b)
    got = send(sent, near(1))
    kept_lag, sent = local(merge_lag_kernel, LAG, 256, side[2], lagged_a, far[2], lagged_b)
    got_lag = send(sent, swap_x_lo)
    kept, sent = local(split_core_kernel, 72, 128, kept, got)
    plain = kept + send(sent, near(2))
    kept, sent = local(split_core_kernel, LAG, 128, kept_lag, got_lag)
    lagged = kept + send(sent, near_shifted(2))
    pieces = jnp.concatenate([plain, lagged], axis=1)

    parts = []
    for move in (2, 1, 3, 0):
        away = (z_high + move - y) % 4
        piece = lax.dynamic_index_in_dim(pieces, away ^ (away // 2), 0, keepdims=False)
        parts.append(send(piece, to_owner(move)))
    return finish(parts)


def solution(mesh):
    return jax.shard_map(
        shards,
        mesh=mesh,
        in_specs=(P("frames", "blocks"), P("frames")),
        out_specs=(P("frames", "blocks"), P("frames", "blocks")),
        check_vma=False,
    )
```

```python
import functools

import jax
import jax.numpy as jnp
from jax import lax
from jax.experimental import pallas as pl
from jax.experimental.pallas import tpu as pltpu
from jax.sharding import PartitionSpec as P


LAG = 64
AXES = ("frames", "blocks")
VMEM = pl.BlockSpec(memory_space=pltpu.VMEM)


def pairs(move):
    out = []
    for frame in range(32):
        for block in range(16):
            target = move(frame // 16, frame % 16, block // 8, (block // 2) % 4, block % 2)
            if target is None:
                continue
            xl, z, xh, y, c = target
            out.append((frame * 16 + block, (xl * 16 + z % 16) * 16 + xh * 8 + (y % 4) * 2 + c))
    return out


def send(value, move):
    return lax.ppermute(value, AXES, pairs(move))


def to_previous(xl, z, xh, y, c):
    frame = xl * 16 + z - 1
    return None if frame < 0 else (frame // 16, frame % 16, xh, y, c)


def up_y(xl, z, xh, y, c):
    return (xl, z, xh, y + 1, c)


def down_y(xl, z, xh, y, c):
    return (xl, z, xh, y - 1, c)


def across_y(xl, z, xh, y, c):
    return (xl, z, xh, y + 2, c)


def swap_x_hi(xl, z, xh, y, c):
    return (xl, z, 1 - xh, y, c)


def swap_core(xl, z, xh, y, c):
    return (xl, z, xh, y, 1 - c)


def swap_x_lo(xl, z, xh, y, c):
    return (1 - xl, z, xh, y, c)


def near(step):
    return lambda xl, z, xh, y, c: (xl, z ^ step, xh, y, c)


def near_shifted(step):
    return lambda xl, z, xh, y, c: (xl, z + step if z & step else z - step, xh, y, c)


def to_owner(step):
    def move(xl, z, xh, y, c):
        high, bit1, bit0 = (z // 4 + step) % 4, (z // 2) % 2, z % 2
        return (xh, high * 4 + c * 2 + bit0, xl, y, bit1)

    return move


def contract(left, right):
    return lax.dot_general(left, right, (((0,), (0,)), ((), ())), preferred_element_type=jnp.float32)


def spread_kernel(with_mask, first_ref, second_ref, tips_ref, mask_ref, tail_ref, out_ref):
    chunk, bodies = 256, (first_ref, second_ref)
    rows = out_ref.shape[0]
    last = rows - chunk

    def store(at, count, lane, value, mask):
        out_ref[pl.ds(at, count), pl.ds(lane, 128)] = value if mask is None else value * mask

    def body(i, carry):
        start = pl.multiple_of(i * chunk, chunk)
        ahead = pl.multiple_of(start + LAG, LAG)
        mask = mask_ref[pl.ds(start, chunk), :]
        for column, ref in enumerate(bodies):
            store(start, chunk, column * 128, ref[pl.ds(start, chunk), :], mask)
            store(start, chunk, 256 + column * 128, ref[pl.ds(ahead, chunk), :], mask)
        if with_mask:
            store(start, chunk, 512, mask, None)
        return carry

    lax.fori_loop(0, last // chunk, body, 0)
    mask, tail = mask_ref[last:, :], tail_ref[...]
    for column, ref in enumerate(bodies):
        store(last, chunk - LAG, column * 128, ref[last : rows - LAG, :], mask)
        store(rows - LAG, LAG, column * 128, ref[rows - LAG :, :], tail)
        store(last, chunk - LAG, 256 + column * 128, ref[last + LAG :, :], mask)
        store(rows - LAG, LAG, 256 + column * 128, tips_ref[column * LAG : (column + 1) * LAG, :], tail)
    if with_mask:
        store(last, chunk - LAG, 512, mask, None)
        store(rows - LAG, LAG, 512, tail, None)


def spread(first, second, tips, mask, tail, with_mask):
    return pl.pallas_call(
        functools.partial(spread_kernel, with_mask),
        out_shape=jax.ShapeDtypeStruct((first.shape[0], 640 if with_mask else 512), jnp.bfloat16),
        in_specs=[VMEM] * 5,
        out_specs=VMEM,
        compiler_params=pltpu.CompilerParams(vmem_limit_bytes=9 << 20),
    )(first, second, tips, mask, tail)


def local_call(kernel, shapes, *args):
    return pl.pallas_call(
        kernel,
        out_shape=tuple(jax.ShapeDtypeStruct(shape, jnp.float32) for shape in shapes),
        in_specs=[VMEM] * len(args),
        out_specs=(VMEM,) * len(shapes),
        compiler_params=pltpu.CompilerParams(vmem_limit_bytes=9 << 20),
    )(*args)


def position():
    frame, block = lax.axis_index("frames"), lax.axis_index("blocks")
    return frame >> 4, frame & 15, block >> 3, (block >> 1) & 3, block & 1


def kept_x():
    x_lo, _, x_hi, _, _ = position()
    return x_lo == x_hi


def low_bit():
    return position()[1] & 1


def arrange_kernel(groups, *refs):
    nears, overs, refs = refs[:groups], refs[groups : 2 * groups], refs[2 * groups :]
    line_near, line_over, plain_keep, plain_send, lag_keep, lag_send = refs
    keep_near, half = kept_x(), low_bit()
    eye = lax.broadcasted_iota(jnp.int32, (128, 128), 0) == lax.broadcasted_iota(jnp.int32, (128, 128), 1)
    row = lax.broadcasted_iota(jnp.int32, (8, 256), 0)

    def wide(value):
        return jnp.broadcast_to(value, (8, value.shape[1]))

    count = wide(jnp.concatenate([line_near[128:129, 512:]] * 2, axis=1))
    lines = [[wide(ref[128:129, at : at + 256]) for at in (0, 256)] for ref in (line_near, line_over)]
    for group, (near_ref, over_ref) in enumerate(zip(nears, overs)):
        sums = jnp.sum(jnp.where(eye, near_ref[:128, 512:], 0.0), axis=0, keepdims=True)
        sums = wide(jnp.concatenate([sums, sums], axis=1))
        for out, take_near in ((plain_keep, keep_near), (plain_send, jnp.logical_not(keep_near))):
            out[group, :128, :] = jnp.where(take_near, near_ref[:128, :256], over_ref[:128, :256])
            now, later = (jnp.where(take_near, a, b) for a, b in zip(*lines))
            out[group, 128:, :] = jnp.where(row == 0, now, jnp.where(row == 1, later, jnp.where(row == 2, sums, count)))
        for out, index in ((lag_keep, half), (lag_send, 1 - half)):
            part = pl.ds(pl.multiple_of(index * LAG, LAG), LAG)
            out[group, :, :256] = near_ref[part, 256:512]
            out[group, :, 256:] = over_ref[part, 256:512]


def arrange(nears, overs, lines):
    groups = len(nears)
    shapes = [(groups, 136, 256)] * 2 + [(groups, LAG, 512)] * 2
    return local_call(functools.partial(arrange_kernel, groups), shapes, *nears, *overs, *lines)


def split_core_kernel(mine, got, keep, send_out):
    _, z, _, _, core = position()
    same = ((z >> 1) & 1) == core
    total = mine[...] + got[...]
    low, high = total[:, :, :128], total[:, :, 128:]
    keep[...] = jnp.where(same, low, high)
    send_out[...] = jnp.where(same, high, low)


def merge_plain_kernel(keep_a, got_a, keep_b, got_b, keep, send_out):
    for out, index in ((keep, low_bit()), (send_out, 1 - low_bit())):
        part = pl.ds(pl.multiple_of(index * LAG, LAG), LAG)
        for at, mine, got in ((0, keep_a, got_a), (3, keep_b, got_b)):
            for group in range(mine.shape[0]):
                out[at + group, :LAG, :] = mine[group, part, :] + got[group, part, :]
                out[at + group, LAG:, :] = mine[group, 128:, :] + got[group, 128:, :]


def merge_lag_kernel(keep_a, got_a, keep_b, got_b, keep, send_out):
    keep_near = kept_x()
    for at, mine, got in ((0, keep_a, got_a), (3, keep_b, got_b)):
        for group in range(mine.shape[0]):
            near_part = mine[group, :, :256] + got[group, :, :256]
            over_part = mine[group, :, 256:] + got[group, :, 256:]
            keep[at + group] = jnp.where(keep_near, near_part, over_part)
            send_out[at + group] = jnp.where(keep_near, over_part, near_part)


def finish_kernel(a_ref, b_ref, c_ref, d_ref, zero_ref, lag_ref):
    total = a_ref[...] + b_ref[...] + c_ref[...] + d_ref[...]
    count = total[LAG + 3 : LAG + 4, :1]
    cols, lags, line = (total[LAG + i : LAG + i + 1] / count for i in range(3))
    row = lax.broadcasted_iota(jnp.int32, (LAG, 128), 0) + low_bit() * LAG
    lane = lax.broadcasted_iota(jnp.int32, (LAG, 128), 1)
    means = jnp.sum(jnp.where(lane == row, jnp.broadcast_to(line, (LAG, 128)), 0.0), axis=1, keepdims=True)
    zero_ref[...] = total[:LAG] / count - means * cols
    lag_ref[...] = total[LAG + 8 :] / count - means * lags


def finish(parts):
    return local_call(finish_kernel, [(LAG, 128)] * 2, *parts)


def shards(frames_data, traj_ids):
    _, z, _, y, _ = position()
    z_high = z >> 2

    own = frames_data
    rows = own.shape[0]
    over_x = send(own, swap_x_hi)
    up, down = send(own, up_y), send(own, down_y)
    over_core = send(own, swap_core)
    beyond = send(own, across_y)
    marks = traj_ids + 1
    mark_rows = jnp.pad(marks[None, :LAG].astype(jnp.bfloat16), ((0, 15), (0, 128 - LAG)))
    tip = send(jnp.concatenate([own[:LAG], over_core[:LAG], mark_rows]), to_previous)
    near_tips = tip[: 2 * LAG]
    over_tips = send(near_tips, swap_x_hi)
    over_both = send(over_x, swap_core)

    def columns(valid):
        return jnp.broadcast_to(valid.astype(jnp.bfloat16)[:, None], (valid.shape[0], 128))

    mask = lax.optimization_barrier(columns(marks[LAG:] == marks[:-LAG]))
    mask_tail = lax.optimization_barrier(columns(tip[2 * LAG, :LAG].astype(jnp.int32) == marks[-LAG:]))

    near_cols = spread(own, over_core, near_tips, mask, mask_tail, True)
    over_cols = spread(over_x, over_both, over_tips, mask, mask_tail, False)
    own_ones = lax.optimization_barrier(jnp.concatenate([own, jnp.ones((rows, 8), jnp.bfloat16)], axis=1))

    sides = (own_ones, down, up)
    side_near = [contract(own_ones, near_cols)]
    side_near += [contract(left, near_cols) for left in sides[1:]]
    side_over = [contract(left, over_cols) for left in sides]
    far_near, far_over = contract(beyond, near_cols), contract(beyond, over_cols)

    lines = (side_near[0], side_over[0])
    side = arrange(side_near, side_over, lines)
    far = arrange([far_near], [far_over], lines)
    plain_a, lagged_a = send(side[1], swap_x_lo), send(side[3], near(1))
    plain_b, lagged_b = send(far[1], swap_x_lo), send(far[3], near(1))

    def local(kernel, count, columns, *args):
        return local_call(kernel, [(4, count, columns)] * 2, *args)

    kept, sent = local(merge_plain_kernel, 72, 256, side[0], plain_a, far[0], plain_b)
    got = send(sent, near(1))
    kept_lag, sent = local(merge_lag_kernel, LAG, 256, side[2], lagged_a, far[2], lagged_b)
    got_lag = send(sent, swap_x_lo)
    kept, sent = local(split_core_kernel, 72, 128, kept, got)
    plain = kept + send(sent, near(2))
    kept, sent = local(split_core_kernel, LAG, 128, kept_lag, got_lag)
    lagged = kept + send(sent, near_shifted(2))
    pieces = jnp.concatenate([plain, lagged], axis=1)

    parts = []
    for move in (2, 1, 3, 0):
        away = (z_high + move - y) % 4
        piece = lax.dynamic_index_in_dim(pieces, away ^ (away // 2), 0, keepdims=False)
        parts.append(send(piece, to_owner(move)))
    return finish(parts)


def solution(mesh):
    return jax.shard_map(
        shards,
        mesh=mesh,
        in_specs=(P("frames", "blocks"), P("frames")),
        out_specs=(P("frames", "blocks"), P("frames", "blocks")),
        check_vma=False,
    )
```

```python
import functools

import jax
import jax.numpy as jnp
from jax import lax
from jax.experimental import pallas as pl
from jax.experimental.pallas import tpu as pltpu
from jax.sharding import PartitionSpec as P


LAG = 64
AXES = ("frames", "blocks")
VMEM = pl.BlockSpec(memory_space=pltpu.VMEM)


def pairs(move):
    out = []
    for frame in range(32):
        for block in range(16):
            target = move(frame // 16, frame % 16, block // 8, (block // 2) % 4, block % 2)
            if target is None:
                continue
            xl, z, xh, y, c = target
            out.append((frame * 16 + block, (xl * 16 + z % 16) * 16 + xh * 8 + (y % 4) * 2 + c))
    return out


def send(value, move):
    return lax.ppermute(value, AXES, pairs(move))


def to_previous(xl, z, xh, y, c):
    frame = xl * 16 + z - 1
    return None if frame < 0 else (frame // 16, frame % 16, xh, y, c)


def up_y(xl, z, xh, y, c):
    return (xl, z, xh, y + 1, c)


def down_y(xl, z, xh, y, c):
    return (xl, z, xh, y - 1, c)


def swap_x_hi(xl, z, xh, y, c):
    return (xl, z, 1 - xh, y, c)


def swap_core(xl, z, xh, y, c):
    return (xl, z, xh, y, 1 - c)


def swap_x_lo(xl, z, xh, y, c):
    return (1 - xl, z, xh, y, c)


def near(step):
    return lambda xl, z, xh, y, c: (xl, z ^ step, xh, y, c)


def near_shifted(step):
    return lambda xl, z, xh, y, c: (xl, z + step if z & step else z - step, xh, y, c)


def to_owner(step):
    def move(xl, z, xh, y, c):
        high, bit1, bit0 = (z // 4 + step) % 4, (z // 2) % 2, z % 2
        return (xh, high * 4 + c * 2 + bit0, xl, y, bit1)

    return move


def contract(left, right):
    return lax.dot_general(left, right, (((0,), (0,)), ((), ())), preferred_element_type=jnp.float32)


def spread_kernel(with_mask, first_ref, second_ref, tips_ref, mask_ref, tail_ref, out_ref):
    chunk, bodies = 256, (first_ref, second_ref)
    rows = out_ref.shape[0]
    last = rows - chunk

    def store(at, count, lane, value, mask):
        out_ref[pl.ds(at, count), pl.ds(lane, 128)] = value if mask is None else value * mask

    def body(i, carry):
        start = pl.multiple_of(i * chunk, chunk)
        ahead = pl.multiple_of(start + LAG, LAG)
        mask = mask_ref[pl.ds(start, chunk), :]
        for column, ref in enumerate(bodies):
            store(start, chunk, column * 128, ref[pl.ds(start, chunk), :], mask)
            store(start, chunk, 256 + column * 128, ref[pl.ds(ahead, chunk), :], mask)
        if with_mask:
            store(start, chunk, 512, mask, None)
        return carry

    lax.fori_loop(0, last // chunk, body, 0)
    mask, tail = mask_ref[last:, :], tail_ref[...]
    for column, ref in enumerate(bodies):
        store(last, chunk - LAG, column * 128, ref[last : rows - LAG, :], mask)
        store(rows - LAG, LAG, column * 128, ref[rows - LAG :, :], tail)
        store(last, chunk - LAG, 256 + column * 128, ref[last + LAG :, :], mask)
        store(rows - LAG, LAG, 256 + column * 128, tips_ref[column * LAG : (column + 1) * LAG, :], tail)
    if with_mask:
        store(last, chunk - LAG, 512, mask, None)
        store(rows - LAG, LAG, 512, tail, None)


def spread(first, second, tips, mask, tail, with_mask):
    return pl.pallas_call(
        functools.partial(spread_kernel, with_mask),
        out_shape=jax.ShapeDtypeStruct((first.shape[0], 640 if with_mask else 512), jnp.bfloat16),
        in_specs=[VMEM] * 5,
        out_specs=VMEM,
        compiler_params=pltpu.CompilerParams(vmem_limit_bytes=9 << 20),
    )(first, second, tips, mask, tail)


def local_call(kernel, shapes, *args):
    return pl.pallas_call(
        kernel,
        out_shape=tuple(jax.ShapeDtypeStruct(shape, jnp.float32) for shape in shapes),
        in_specs=[VMEM] * len(args),
        out_specs=(VMEM,) * len(shapes),
        compiler_params=pltpu.CompilerParams(vmem_limit_bytes=9 << 20),
    )(*args)


def position():
    frame, block = lax.axis_index("frames"), lax.axis_index("blocks")
    return frame >> 4, frame & 15, block >> 3, (block >> 1) & 3, block & 1


def kept_x():
    x_lo, _, x_hi, _, _ = position()
    return x_lo == x_hi


def low_bit():
    return position()[1] & 1


def arrange_kernel(groups, *refs):
    nears, overs, refs = refs[:groups], refs[groups : 2 * groups], refs[2 * groups :]
    line_near, line_over, plain_keep, plain_send, lag_keep, lag_send = refs
    keep_near, half = kept_x(), low_bit()
    eye = lax.broadcasted_iota(jnp.int32, (128, 128), 0) == lax.broadcasted_iota(jnp.int32, (128, 128), 1)
    row = lax.broadcasted_iota(jnp.int32, (8, 256), 0)

    def wide(value):
        return jnp.broadcast_to(value, (8, value.shape[1]))

    count = wide(jnp.concatenate([line_near[128:129, 512:]] * 2, axis=1))
    lines = [[wide(ref[128:129, at : at + 256]) for at in (0, 256)] for ref in (line_near, line_over)]
    for group, (near_ref, over_ref) in enumerate(zip(nears, overs)):
        sums = jnp.sum(jnp.where(eye, near_ref[:128, 512:], 0.0), axis=0, keepdims=True)
        sums = wide(jnp.concatenate([sums, sums], axis=1))
        for out, take_near in ((plain_keep, keep_near), (plain_send, jnp.logical_not(keep_near))):
            out[group, :128, :] = jnp.where(take_near, near_ref[:128, :256], over_ref[:128, :256])
            now, later = (jnp.where(take_near, a, b) for a, b in zip(*lines))
            out[group, 128:, :] = jnp.where(row == 0, now, jnp.where(row == 1, later, jnp.where(row == 2, sums, count)))
        for out, index in ((lag_keep, half), (lag_send, 1 - half)):
            part = pl.ds(pl.multiple_of(index * LAG, LAG), LAG)
            out[group, :, :256] = near_ref[part, 256:512]
            out[group, :, 256:] = over_ref[part, 256:512]


def arrange(nears, overs, lines):
    groups = len(nears)
    shapes = [(groups, 136, 256)] * 2 + [(groups, LAG, 512)] * 2
    return local_call(functools.partial(arrange_kernel, groups), shapes, *nears, *overs, *lines)


def split_core_kernel(mine, got, keep, send_out):
    _, z, _, _, core = position()
    same = ((z >> 1) & 1) == core
    total = mine[...] + got[...]
    low, high = total[:, :, :128], total[:, :, 128:]
    keep[...] = jnp.where(same, low, high)
    send_out[...] = jnp.where(same, high, low)


def merge_plain_kernel(keep_a, got_a, keep_b, got_b, keep, send_out):
    for out, index in ((keep, low_bit()), (send_out, 1 - low_bit())):
        part = pl.ds(pl.multiple_of(index * LAG, LAG), LAG)
        for at, mine, got in ((0, keep_a, got_a), (3, keep_b, got_b)):
            for group in range(mine.shape[0]):
                out[at + group, :LAG, :] = mine[group, part, :] + got[group, part, :]
                out[at + group, LAG:, :] = mine[group, 128:, :] + got[group, 128:, :]


def merge_lag_kernel(keep_a, got_a, keep_b, got_b, keep, send_out):
    keep_near = kept_x()
    for at, mine, got in ((0, keep_a, got_a), (3, keep_b, got_b)):
        for group in range(mine.shape[0]):
            near_part = mine[group, :, :256] + got[group, :, :256]
            over_part = mine[group, :, 256:] + got[group, :, 256:]
            keep[at + group] = jnp.where(keep_near, near_part, over_part)
            send_out[at + group] = jnp.where(keep_near, over_part, near_part)


def finish_kernel(a_ref, b_ref, c_ref, d_ref, zero_ref, lag_ref):
    total = a_ref[...] + b_ref[...] + c_ref[...] + d_ref[...]
    count = total[LAG + 3 : LAG + 4, :1]
    cols, lags, line = (total[LAG + i : LAG + i + 1] / count for i in range(3))
    row = lax.broadcasted_iota(jnp.int32, (LAG, 128), 0) + low_bit() * LAG
    lane = lax.broadcasted_iota(jnp.int32, (LAG, 128), 1)
    means = jnp.sum(jnp.where(lane == row, jnp.broadcast_to(line, (LAG, 128)), 0.0), axis=1, keepdims=True)
    zero_ref[...] = total[:LAG] / count - means * cols
    lag_ref[...] = total[LAG + 8 :] / count - means * lags


def finish(parts):
    return local_call(finish_kernel, [(LAG, 128)] * 2, *parts)


def shards(frames_data, traj_ids):
    _, z, _, y, _ = position()
    z_high = z >> 2

    own = frames_data
    rows = own.shape[0]
    over_x = send(own, swap_x_hi)
    up, down = send(own, up_y), send(own, down_y)
    over_core = send(own, swap_core)
    marks = traj_ids + 1
    mark_rows = jnp.pad(marks[None, :LAG].astype(jnp.bfloat16), ((0, 15), (0, 128 - LAG)))
    tip = send(jnp.concatenate([own[:LAG], over_core[:LAG], mark_rows]), to_previous)
    near_tips = tip[: 2 * LAG]
    over_tips = send(near_tips, swap_x_hi)
    over_both = send(over_x, swap_core)
    middle = rows // 2
    up_part, down_part = up[:middle], down[middle:]
    far_a, far_b = send(up_part, up_y), send(down_part, down_y)

    def columns(valid):
        return jnp.broadcast_to(valid.astype(jnp.bfloat16)[:, None], (valid.shape[0], 128))

    mask = lax.optimization_barrier(columns(marks[LAG:] == marks[:-LAG]))
    mask_tail = lax.optimization_barrier(columns(tip[2 * LAG, :LAG].astype(jnp.int32) == marks[-LAG:]))

    near_cols = spread(own, over_core, near_tips, mask, mask_tail, True)
    over_cols = spread(over_x, over_both, over_tips, mask, mask_tail, False)
    own_ones = lax.optimization_barrier(jnp.concatenate([own, jnp.ones((rows, 8), jnp.bfloat16)], axis=1))

    sides = (own_ones, down, up)
    side_near = [contract(own_ones, near_cols)]
    side_near += [contract(left, near_cols) for left in sides[1:]]
    side_over = [contract(left, over_cols) for left in sides]
    beyond = jnp.concatenate([far_a, far_b])
    far_near, far_over = contract(beyond, near_cols), contract(beyond, over_cols)

    lines = (side_near[0], side_over[0])
    side = arrange(side_near, side_over, lines)
    far = arrange([far_near], [far_over], lines)
    plain_a, lagged_a = send(side[1], swap_x_lo), send(side[3], near(1))
    plain_b, lagged_b = send(far[1], swap_x_lo), send(far[3], near(1))

    def local(kernel, count, columns, *args):
        return local_call(kernel, [(4, count, columns)] * 2, *args)

    kept, sent = local(merge_plain_kernel, 72, 256, side[0], plain_a, far[0], plain_b)
    got = send(sent, near(1))
    kept_lag, sent = local(merge_lag_kernel, LAG, 256, side[2], lagged_a, far[2], lagged_b)
    got_lag = send(sent, swap_x_lo)
    kept, sent = local(split_core_kernel, 72, 128, kept, got)
    plain = kept + send(sent, near(2))
    kept, sent = local(split_core_kernel, LAG, 128, kept_lag, got_lag)
    lagged = kept + send(sent, near_shifted(2))
    pieces = jnp.concatenate([plain, lagged], axis=1)

    parts = []
    for move in (2, 1, 3, 0):
        away = (z_high + move - y) % 4
        piece = lax.dynamic_index_in_dim(pieces, away ^ (away // 2), 0, keepdims=False)
        parts.append(send(piece, to_owner(move)))
    return finish(parts)


def solution(mesh):
    return jax.shard_map(
        shards,
        mesh=mesh,
        in_specs=(P("frames", "blocks"), P("frames")),
        out_specs=(P("frames", "blocks"), P("frames", "blocks")),
        check_vma=False,
    )
```

```python
import functools

import jax
import jax.numpy as jnp
from jax import lax
from jax.experimental import pallas as pl
from jax.experimental.pallas import tpu as pltpu
from jax.sharding import PartitionSpec as P


LAG = 64
AXES = ("frames", "blocks")
VMEM = pl.BlockSpec(memory_space=pltpu.VMEM)


def pairs(move):
    out = []
    for frame in range(32):
        for block in range(16):
            target = move(frame // 16, frame % 16, block // 8, (block // 2) % 4, block % 2)
            if target is None:
                continue
            xl, z, xh, y, c = target
            out.append((frame * 16 + block, (xl * 16 + z % 16) * 16 + xh * 8 + (y % 4) * 2 + c))
    return out


def send(value, move):
    return lax.ppermute(value, AXES, pairs(move))


def to_previous(xl, z, xh, y, c):
    frame = xl * 16 + z - 1
    return None if frame < 0 else (frame // 16, frame % 16, xh, y, c)


def up_y(xl, z, xh, y, c):
    return (xl, z, xh, y + 1, c)


def down_y(xl, z, xh, y, c):
    return (xl, z, xh, y - 1, c)


def swap_x_hi(xl, z, xh, y, c):
    return (xl, z, 1 - xh, y, c)


def swap_core(xl, z, xh, y, c):
    return (xl, z, xh, y, 1 - c)


def first_step(xl, z, xh, y, c):
    return (xl, z ^ 1, xh, y, c) if c else (1 - xl, z, xh, y, c)


def second_step(xl, z, xh, y, c):
    return (1 - xl, z, xh, y, c) if c else (xl, z ^ 1, xh, y, c)


def third_step(xl, z, xh, y, c):
    if c:
        return (xl, z + 2 if z & 2 else z - 2, xh, y, c)
    return (xl, z ^ 2, xh, y, c)


def to_owner(step):
    def move(xl, z, xh, y, c):
        high, bit1, bit0 = (z // 4 + step) % 4, (z // 2) % 2, z % 2
        return (xh, high * 4 + c * 2 + bit0, xl, y, bit1)

    return move


def contract(left, right):
    return lax.dot_general(left, right, (((0,), (0,)), ((), ())), preferred_element_type=jnp.float32)


def spread_kernel(with_mask, first_ref, second_ref, tips_ref, mask_ref, tail_ref, out_ref):
    chunk, bodies = 256, (first_ref, second_ref)
    rows = out_ref.shape[0]
    last = rows - chunk

    def store(at, count, lane, value, mask):
        out_ref[pl.ds(at, count), pl.ds(lane, 128)] = value if mask is None else value * mask

    def body(i, carry):
        start = pl.multiple_of(i * chunk, chunk)
        ahead = pl.multiple_of(start + LAG, LAG)
        mask = mask_ref[pl.ds(start, chunk), :]
        for column, ref in enumerate(bodies):
            store(start, chunk, column * 128, ref[pl.ds(start, chunk), :], mask)
            store(start, chunk, 256 + column * 128, ref[pl.ds(ahead, chunk), :], mask)
        if with_mask:
            store(start, chunk, 512, mask, None)
        return carry

    lax.fori_loop(0, last // chunk, body, 0)
    mask, tail = mask_ref[last:, :], tail_ref[...]
    for column, ref in enumerate(bodies):
        store(last, chunk - LAG, column * 128, ref[last : rows - LAG, :], mask)
        store(rows - LAG, LAG, column * 128, ref[rows - LAG :, :], tail)
        store(last, chunk - LAG, 256 + column * 128, ref[last + LAG :, :], mask)
        store(rows - LAG, LAG, 256 + column * 128, tips_ref[column * LAG : (column + 1) * LAG, :], tail)
    if with_mask:
        store(last, chunk - LAG, 512, mask, None)
        store(rows - LAG, LAG, 512, tail, None)


def spread(first, second, tips, mask, tail, with_mask):
    return pl.pallas_call(
        functools.partial(spread_kernel, with_mask),
        out_shape=jax.ShapeDtypeStruct((first.shape[0], 640 if with_mask else 512), jnp.bfloat16),
        in_specs=[VMEM] * 5,
        out_specs=VMEM,
        compiler_params=pltpu.CompilerParams(vmem_limit_bytes=9 << 20),
    )(first, second, tips, mask, tail)


def local_call(kernel, shapes, *args):
    return pl.pallas_call(
        kernel,
        out_shape=tuple(jax.ShapeDtypeStruct(shape, jnp.float32) for shape in shapes),
        in_specs=[VMEM] * len(args),
        out_specs=(VMEM,) * len(shapes),
        compiler_params=pltpu.CompilerParams(vmem_limit_bytes=9 << 20),
    )(*args)


def position():
    frame, block = lax.axis_index("frames"), lax.axis_index("blocks")
    return frame >> 4, frame & 15, block >> 3, (block >> 1) & 3, block & 1


def kept_x():
    x_lo, _, x_hi, _, _ = position()
    return x_lo == x_hi


def low_bit():
    return position()[1] & 1


def arrange_kernel(groups, *refs):
    nears, overs, (line_near, line_over, keep, send_out) = refs[:groups], refs[groups : 2 * groups], refs[2 * groups :]
    keep_near, half, core = kept_x(), low_bit(), position()[4]
    eye = lax.broadcasted_iota(jnp.int32, (128, 128), 0) == lax.broadcasted_iota(jnp.int32, (128, 128), 1)
    row = lax.broadcasted_iota(jnp.int32, (8, 256), 0)

    def wide(value):
        return jnp.broadcast_to(value, (8, value.shape[1]))

    count = wide(jnp.concatenate([line_near[128:129, 512:]] * 2, axis=1))
    lines = [[wide(ref[128:129, at : at + 256]) for at in (0, 256)] for ref in (line_near, line_over)]
    for group, (near_ref, over_ref) in enumerate(zip(nears, overs)):
        sums = jnp.sum(jnp.where(eye, near_ref[:128, 512:], 0.0), axis=0, keepdims=True)
        sums = jnp.where(row == 2, wide(jnp.concatenate([sums, sums], axis=1)), count)
        extras = [jnp.where(row == 0, now, jnp.where(row == 1, later, sums)) for now, later in lines]

        @pl.when(core == 0)
        def _(group=group, near_ref=near_ref, over_ref=over_ref, extras=extras):
            for out, take_near in ((keep, keep_near), (send_out, jnp.logical_not(keep_near))):
                for part in range(2):
                    lanes = slice(part * 256, part * 256 + 256)
                    value = jnp.where(take_near, near_ref[:128, lanes], over_ref[:128, lanes])
                    out[group, part * 128 : part * 128 + 128, :] = value
                extra = jnp.where(take_near, extras[0], extras[1])
                out[group, 256:264, :] = extra
                out[group, 264:, :] = extra

        @pl.when(core == 1)
        def _(group=group, near_ref=near_ref, over_ref=over_ref, extras=extras):
            for out, index in ((keep, half), (send_out, 1 - half)):
                rows = pl.ds(pl.multiple_of(index * LAG, LAG), LAG)
                for part in range(2):
                    lanes = slice(part * 256, part * 256 + 256)
                    out[group, part * 128 : part * 128 + LAG, :] = near_ref[rows, lanes]
                    out[group, part * 128 + LAG : part * 128 + 128, :] = over_ref[rows, lanes]
                out[group, 256:264, :] = extras[0]
                out[group, 264:, :] = extras[1]


def arrange(nears, overs, lines):
    groups = len(nears)
    return local_call(functools.partial(arrange_kernel, groups), [(groups, 272, 256)] * 2, *nears, *overs, *lines)


def merge_kernel(keep_a, got_a, keep_b, got_b, keep, send_out):
    core = position()[4]
    mine_index = jnp.where(core == 0, low_bit(), jnp.where(kept_x(), 0, 1))
    for out, index in ((keep, mine_index), (send_out, 1 - mine_index)):
        places = (
            (0, LAG, pl.multiple_of(index * LAG, LAG)),
            (LAG, 8, pl.multiple_of(256 + jnp.where(core == 0, 0, index) * 8, 8)),
            (LAG + 8, LAG, pl.multiple_of(128 + index * LAG, LAG)),
        )
        for at, mine, got in ((0, keep_a, got_a), (3, keep_b, got_b)):
            for group in range(mine.shape[0]):
                for row, count, start in places:
                    rows = pl.ds(start, count)
                    out[at + group, row : row + count, :] = mine[group, rows, :] + got[group, rows, :]


def split_core_kernel(mine, got, keep, send_out):
    _, z, _, _, core = position()
    same = ((z >> 1) & 1) == core
    total = mine[...] + got[...]
    low, high = total[:, :, :128], total[:, :, 128:]
    keep[...] = jnp.where(same, low, high)
    send_out[...] = jnp.where(same, high, low)


def finish_kernel(a_ref, b_ref, c_ref, d_ref, zero_ref, lag_ref):
    total = a_ref[...] + b_ref[...] + c_ref[...] + d_ref[...]
    count = total[LAG + 3 : LAG + 4, :1]
    cols, lags, line = (total[LAG + i : LAG + i + 1] / count for i in range(3))
    row = lax.broadcasted_iota(jnp.int32, (LAG, 128), 0) + low_bit() * LAG
    lane = lax.broadcasted_iota(jnp.int32, (LAG, 128), 1)
    means = jnp.sum(jnp.where(lane == row, jnp.broadcast_to(line, (LAG, 128)), 0.0), axis=1, keepdims=True)
    zero_ref[...] = total[:LAG] / count - means * cols
    lag_ref[...] = total[LAG + 8 :] / count - means * lags


def finish(parts):
    return local_call(finish_kernel, [(LAG, 128)] * 2, *parts)


def shards(frames_data, traj_ids):
    _, z, _, y, _ = position()
    z_high = z >> 2

    own = frames_data
    rows = own.shape[0]
    over_x = send(own, swap_x_hi)
    up, down = send(own, up_y), send(own, down_y)
    over_core = send(own, swap_core)
    marks = traj_ids + 1
    mark_rows = jnp.pad(marks[None, :LAG].astype(jnp.bfloat16), ((0, 15), (0, 128 - LAG)))
    tip = send(jnp.concatenate([own[:LAG], over_core[:LAG], mark_rows]), to_previous)
    near_tips = tip[: 2 * LAG]
    over_tips = send(near_tips, swap_x_hi)
    over_both = send(over_x, swap_core)
    middle = rows // 2
    up_part, down_part = up[:middle], down[middle:]
    far_a, far_b = send(up_part, up_y), send(down_part, down_y)

    def columns(valid):
        return jnp.broadcast_to(valid.astype(jnp.bfloat16)[:, None], (valid.shape[0], 128))

    mask = lax.optimization_barrier(columns(marks[LAG:] == marks[:-LAG]))
    mask_tail = lax.optimization_barrier(columns(tip[2 * LAG, :LAG].astype(jnp.int32) == marks[-LAG:]))

    near_cols = spread(own, over_core, near_tips, mask, mask_tail, True)
    over_cols = spread(over_x, over_both, over_tips, mask, mask_tail, False)
    own_ones = lax.optimization_barrier(jnp.concatenate([own, jnp.ones((rows, 8), jnp.bfloat16)], axis=1))

    sides = (own_ones, down, up)
    side_near = [contract(own_ones, near_cols)]
    side_near += [contract(left, near_cols) for left in sides[1:]]
    side_over = [contract(left, over_cols) for left in sides]
    beyond = jnp.concatenate([far_a, far_b])
    far_near, far_over = contract(beyond, near_cols), contract(beyond, over_cols)

    lines = (side_near[0], side_over[0])
    side = arrange(side_near, side_over, lines)
    far = arrange([far_near], [far_over], lines)
    got_a, got_b = send(side[1], first_step), send(far[1], first_step)
    kept, sent = local_call(merge_kernel, [(4, 136, 256)] * 2, side[0], got_a, far[0], got_b)
    got = send(sent, second_step)
    kept, sent = local_call(split_core_kernel, [(4, 136, 128)] * 2, kept, got)
    pieces = kept + send(sent, third_step)

    parts = []
    for move in (2, 1, 3, 0):
        away = (z_high + move - y) % 4
        piece = lax.dynamic_index_in_dim(pieces, away ^ (away // 2), 0, keepdims=False)
        parts.append(send(piece, to_owner(move)))
    return finish(parts)


def solution(mesh):
    return jax.shard_map(
        shards,
        mesh=mesh,
        in_specs=(P("frames", "blocks"), P("frames")),
        out_specs=(P("frames", "blocks"), P("frames", "blocks")),
        check_vma=False,
    )
```

```python
import functools

import jax
import jax.numpy as jnp
from jax import lax
from jax.experimental import pallas as pl
from jax.experimental.pallas import tpu as pltpu
from jax.sharding import PartitionSpec as P


LAG = 64
AXES = ("frames", "blocks")
VMEM = pl.BlockSpec(memory_space=pltpu.VMEM)


def pairs(move):
    out = []
    for frame in range(32):
        for block in range(16):
            target = move(frame // 16, frame % 16, block // 8, (block // 2) % 4, block % 2)
            if target is None:
                continue
            xl, z, xh, y, c = target
            out.append((frame * 16 + block, (xl * 16 + z % 16) * 16 + xh * 8 + (y % 4) * 2 + c))
    return out


def send(value, move):
    return lax.ppermute(value, AXES, pairs(move))


def to_previous(xl, z, xh, y, c):
    frame = xl * 16 + z - 1
    return None if frame < 0 else (frame // 16, frame % 16, xh, y, c)


def up_y(xl, z, xh, y, c):
    return (xl, z, xh, y + 1, c)


def down_y(xl, z, xh, y, c):
    return (xl, z, xh, y - 1, c)


def swap_x_hi(xl, z, xh, y, c):
    return (xl, z, 1 - xh, y, c)


def swap_core(xl, z, xh, y, c):
    return (xl, z, xh, y, 1 - c)


def swap_x_lo(xl, z, xh, y, c):
    return (1 - xl, z, xh, y, c)


def near(step):
    return lambda xl, z, xh, y, c: (xl, z ^ step, xh, y, c)


def near_shifted(step):
    return lambda xl, z, xh, y, c: (xl, z + step if z & step else z - step, xh, y, c)


def to_owner(step):
    def move(xl, z, xh, y, c):
        high, bit1, bit0 = (z // 4 + step) % 4, (z // 2) % 2, z % 2
        return (xh, high * 4 + c * 2 + bit0, xl, y, bit1)

    return move


def contract(left, right):
    return lax.dot_general(left, right, (((0,), (0,)), ((), ())), preferred_element_type=jnp.float32)


def spread_kernel(with_mask, first_ref, second_ref, tips_ref, mask_ref, tail_ref, out_ref):
    chunk, bodies = 256, (first_ref, second_ref)
    rows = out_ref.shape[0]
    last = rows - chunk

    def store(at, count, lane, value, mask):
        out_ref[pl.ds(at, count), pl.ds(lane, 128)] = value if mask is None else value * mask

    def body(i, carry):
        start = pl.multiple_of(i * chunk, chunk)
        ahead = pl.multiple_of(start + LAG, LAG)
        mask = mask_ref[pl.ds(start, chunk), :]
        for column, ref in enumerate(bodies):
            store(start, chunk, column * 128, ref[pl.ds(start, chunk), :], mask)
            store(start, chunk, 256 + column * 128, ref[pl.ds(ahead, chunk), :], mask)
        if with_mask:
            store(start, chunk, 512, mask, None)
        return carry

    lax.fori_loop(0, last // chunk, body, 0)
    mask, tail = mask_ref[last:, :], tail_ref[...]
    for column, ref in enumerate(bodies):
        store(last, chunk - LAG, column * 128, ref[last : rows - LAG, :], mask)
        store(rows - LAG, LAG, column * 128, ref[rows - LAG :, :], tail)
        store(last, chunk - LAG, 256 + column * 128, ref[last + LAG :, :], mask)
        store(rows - LAG, LAG, 256 + column * 128, tips_ref[column * LAG : (column + 1) * LAG, :], tail)
    if with_mask:
        store(last, chunk - LAG, 512, mask, None)
        store(rows - LAG, LAG, 512, tail, None)


def spread(first, second, tips, mask, tail, with_mask):
    return pl.pallas_call(
        functools.partial(spread_kernel, with_mask),
        out_shape=jax.ShapeDtypeStruct((first.shape[0], 640 if with_mask else 512), jnp.bfloat16),
        in_specs=[VMEM] * 5,
        out_specs=VMEM,
        compiler_params=pltpu.CompilerParams(vmem_limit_bytes=9 << 20),
    )(first, second, tips, mask, tail)


def local_call(kernel, shapes, *args):
    return pl.pallas_call(
        kernel,
        out_shape=tuple(jax.ShapeDtypeStruct(shape, jnp.float32) for shape in shapes),
        in_specs=[VMEM] * len(args),
        out_specs=(VMEM,) * len(shapes),
        compiler_params=pltpu.CompilerParams(vmem_limit_bytes=9 << 20),
    )(*args)


def position():
    frame, block = lax.axis_index("frames"), lax.axis_index("blocks")
    return frame >> 4, frame & 15, block >> 3, (block >> 1) & 3, block & 1


def kept_x():
    x_lo, _, x_hi, _, _ = position()
    return x_lo == x_hi


def low_bit():
    return position()[1] & 1


def arrange_kernel(groups, *refs):
    nears, overs, refs = refs[:groups], refs[groups : 2 * groups], refs[2 * groups :]
    line_near, line_over, plain_keep, plain_send, lag_keep, lag_send = refs
    keep_near, half = kept_x(), low_bit()
    eye = lax.broadcasted_iota(jnp.int32, (128, 128), 0) == lax.broadcasted_iota(jnp.int32, (128, 128), 1)
    row = lax.broadcasted_iota(jnp.int32, (8, 256), 0)

    def wide(value):
        return jnp.broadcast_to(value, (8, value.shape[1]))

    count = wide(jnp.concatenate([line_near[128:129, 512:]] * 2, axis=1))
    lines = [[wide(ref[128:129, at : at + 256]) for at in (0, 256)] for ref in (line_near, line_over)]
    for group, (near_ref, over_ref) in enumerate(zip(nears, overs)):
        sums = jnp.sum(jnp.where(eye, near_ref[:128, 512:], 0.0), axis=0, keepdims=True)
        sums = wide(jnp.concatenate([sums, sums], axis=1))
        for out, take_near in ((plain_keep, keep_near), (plain_send, jnp.logical_not(keep_near))):
            out[group, :128, :] = jnp.where(take_near, near_ref[:128, :256], over_ref[:128, :256])
            now, later = (jnp.where(take_near, a, b) for a, b in zip(*lines))
            out[group, 128:, :] = jnp.where(row == 0, now, jnp.where(row == 1, later, jnp.where(row == 2, sums, count)))
        for out, index in ((lag_keep, half), (lag_send, 1 - half)):
            part = pl.ds(pl.multiple_of(index * LAG, LAG), LAG)
            out[group, :, :256] = near_ref[part, 256:512]
            out[group, :, 256:] = over_ref[part, 256:512]


def arrange(nears, overs, lines):
    groups = len(nears)
    shapes = [(groups, 136, 256)] * 2 + [(groups, LAG, 512)] * 2
    return local_call(functools.partial(arrange_kernel, groups), shapes, *nears, *overs, *lines)


def split_core_kernel(mine, got, keep, send_out):
    _, z, _, _, core = position()
    same = ((z >> 1) & 1) == core
    total = mine[...] + got[...]
    low, high = total[:, :, :128], total[:, :, 128:]
    keep[...] = jnp.where(same, low, high)
    send_out[...] = jnp.where(same, high, low)


def merge_plain_kernel(keep_a, got_a, keep_b, got_b, keep, send_out):
    for out, index in ((keep, low_bit()), (send_out, 1 - low_bit())):
        part = pl.ds(pl.multiple_of(index * LAG, LAG), LAG)
        for at, mine, got in ((0, keep_a, got_a), (3, keep_b, got_b)):
            for group in range(mine.shape[0]):
                out[at + group, :LAG, :] = mine[group, part, :] + got[group, part, :]
                out[at + group, LAG:, :] = mine[group, 128:, :] + got[group, 128:, :]


def merge_lag_kernel(keep_a, got_a, keep_b, got_b, keep, send_out):
    keep_near = kept_x()
    for at, mine, got in ((0, keep_a, got_a), (3, keep_b, got_b)):
        for group in range(mine.shape[0]):
            near_part = mine[group, :, :256] + got[group, :, :256]
            over_part = mine[group, :, 256:] + got[group, :, 256:]
            keep[at + group] = jnp.where(keep_near, near_part, over_part)
            send_out[at + group] = jnp.where(keep_near, over_part, near_part)


def finish_kernel(a_ref, b_ref, c_ref, d_ref, zero_ref, lag_ref):
    total = a_ref[...] + b_ref[...] + c_ref[...] + d_ref[...]
    count = total[LAG + 3 : LAG + 4, :1]
    cols, lags, line = (total[LAG + i : LAG + i + 1] / count for i in range(3))
    row = lax.broadcasted_iota(jnp.int32, (LAG, 128), 0) + low_bit() * LAG
    lane = lax.broadcasted_iota(jnp.int32, (LAG, 128), 1)
    means = jnp.sum(jnp.where(lane == row, jnp.broadcast_to(line, (LAG, 128)), 0.0), axis=1, keepdims=True)
    zero_ref[...] = total[:LAG] / count - means * cols
    lag_ref[...] = total[LAG + 8 :] / count - means * lags


def finish(parts):
    return local_call(finish_kernel, [(LAG, 128)] * 2, *parts)


def shards(frames_data, traj_ids):
    _, z, _, y, _ = position()
    z_high = z >> 2

    own = frames_data
    rows = own.shape[0]
    over_x = send(own, swap_x_hi)
    up, down = send(own, up_y), send(own, down_y)
    over_core = send(own, swap_core)
    mark_rows = jnp.pad((traj_ids[None, :LAG] + 1).astype(jnp.bfloat16), ((0, 15), (0, 128 - LAG)))
    tip = send(jnp.concatenate([own[:LAG], over_core[:LAG], mark_rows]), to_previous)
    near_tips = tip[: 2 * LAG]
    over_tips = send(near_tips, swap_x_hi)
    over_both = send(over_x, swap_core)
    middle = rows // 2
    up_part, down_part = up[:middle], down[middle:]
    far_a, far_b = send(up_part, up_y), send(down_part, down_y)

    def columns(valid):
        return jnp.broadcast_to(valid.astype(jnp.bfloat16)[:, None], (valid.shape[0], 128))

    mask = lax.optimization_barrier(columns(traj_ids[LAG:] == traj_ids[:-LAG]))
    mask_tail = lax.optimization_barrier(columns(tip[2 * LAG, :LAG].astype(jnp.int32) == traj_ids[-LAG:] + 1))

    near_cols = spread(own, over_core, near_tips, mask, mask_tail, True)
    over_cols = spread(over_x, over_both, over_tips, mask, mask_tail, False)
    own_ones = lax.optimization_barrier(jnp.concatenate([own, jnp.ones((rows, 8), jnp.bfloat16)], axis=1))

    sides = (own_ones, down, up)
    side_near = [contract(own_ones, near_cols)]
    side_near += [contract(left, near_cols) for left in sides[1:]]
    side_over = [contract(left, over_cols) for left in sides]
    beyond = jnp.concatenate([far_a, far_b])
    far_near, far_over = contract(beyond, near_cols), contract(beyond, over_cols)

    lines = (side_near[0], side_over[0])
    side = arrange(side_near, side_over, lines)
    far = arrange([far_near], [far_over], lines)
    plain_a, lagged_a = send(side[1], swap_x_lo), send(side[3], near(1))
    plain_b, lagged_b = send(far[1], swap_x_lo), send(far[3], near(1))

    def local(kernel, count, columns, *args):
        return local_call(kernel, [(4, count, columns)] * 2, *args)

    kept, sent = local(merge_plain_kernel, 72, 256, side[0], plain_a, far[0], plain_b)
    got = send(sent, near(1))
    kept_lag, sent = local(merge_lag_kernel, LAG, 256, side[2], lagged_a, far[2], lagged_b)
    got_lag = send(sent, swap_x_lo)
    kept, sent = local(split_core_kernel, 72, 128, kept, got)
    plain = kept + send(sent, near(2))
    kept, sent = local(split_core_kernel, LAG, 128, kept_lag, got_lag)
    lagged = kept + send(sent, near_shifted(2))
    pieces = jnp.concatenate([plain, lagged], axis=1)

    parts = []
    for move in (2, 1, 3, 0):
        away = (z_high + move - y) % 4
        piece = lax.dynamic_index_in_dim(pieces, away ^ (away // 2), 0, keepdims=False)
        parts.append(send(piece, to_owner(move)))
    return finish(parts)


def solution(mesh):
    return jax.shard_map(
        shards,
        mesh=mesh,
        in_specs=(P("frames", "blocks"), P("frames")),
        out_specs=(P("frames", "blocks"), P("frames", "blocks")),
        check_vma=False,
    )
```

```python
import functools

import jax
import jax.numpy as jnp
from jax import lax
from jax.experimental import pallas as pl
from jax.experimental.pallas import tpu as pltpu
from jax.sharding import PartitionSpec as P


LAG = 64
AXES = ("frames", "blocks")
VMEM = pl.BlockSpec(memory_space=pltpu.VMEM)


def pairs(move):
    out = []
    for frame in range(32):
        for block in range(16):
            target = move(frame // 16, frame % 16, block // 8, (block // 2) % 4, block % 2)
            if target is None:
                continue
            xl, z, xh, y, c = target
            out.append((frame * 16 + block, (xl * 16 + z % 16) * 16 + xh * 8 + (y % 4) * 2 + c))
    return out


def send(value, move):
    return lax.ppermute(value, AXES, pairs(move))


def to_previous(xl, z, xh, y, c):
    frame = xl * 16 + z - 1
    return None if frame < 0 else (frame // 16, frame % 16, xh, y, c)


def up_y(xl, z, xh, y, c):
    return (xl, z, xh, y + 1, c)


def down_y(xl, z, xh, y, c):
    return (xl, z, xh, y - 1, c)


def swap_x_hi(xl, z, xh, y, c):
    return (xl, z, 1 - xh, y, c)


def swap_core(xl, z, xh, y, c):
    return (xl, z, xh, y, 1 - c)


def swap_x_lo(xl, z, xh, y, c):
    return (1 - xl, z, xh, y, c)


def near(step):
    return lambda xl, z, xh, y, c: (xl, z ^ step, xh, y, c)


def near_shifted(step):
    return lambda xl, z, xh, y, c: (xl, z + step if z & step else z - step, xh, y, c)


def to_owner(step):
    def move(xl, z, xh, y, c):
        high, bit1, bit0 = (z // 4 + step) % 4, (z // 2) % 2, z % 2
        return (xh, high * 4 + c * 2 + bit0, xl, y, bit1)

    return move


def contract(left, right):
    return lax.dot_general(left, right, (((0,), (0,)), ((), ())), preferred_element_type=jnp.float32)


def spread_kernel(with_mask, first_ref, second_ref, tips_ref, mask_ref, tail_ref, out_ref):
    chunk, bodies = 256, (first_ref, second_ref)
    rows = out_ref.shape[0]
    last = rows - chunk

    def store(at, count, lane, value, mask):
        out_ref[pl.ds(at, count), pl.ds(lane, 128)] = value if mask is None else value * mask

    def body(i, carry):
        start = pl.multiple_of(i * chunk, chunk)
        ahead = pl.multiple_of(start + LAG, LAG)
        mask = mask_ref[pl.ds(start, chunk), :]
        for column, ref in enumerate(bodies):
            store(start, chunk, column * 128, ref[pl.ds(start, chunk), :], mask)
            store(start, chunk, 256 + column * 128, ref[pl.ds(ahead, chunk), :], mask)
        if with_mask:
            store(start, chunk, 512, mask, None)
        return carry

    lax.fori_loop(0, last // chunk, body, 0)
    mask, tail = mask_ref[last:, :], tail_ref[...]
    for column, ref in enumerate(bodies):
        store(last, chunk - LAG, column * 128, ref[last : rows - LAG, :], mask)
        store(rows - LAG, LAG, column * 128, ref[rows - LAG :, :], tail)
        store(last, chunk - LAG, 256 + column * 128, ref[last + LAG :, :], mask)
        store(rows - LAG, LAG, 256 + column * 128, tips_ref[column * LAG : (column + 1) * LAG, :], tail)
    if with_mask:
        store(last, chunk - LAG, 512, mask, None)
        store(rows - LAG, LAG, 512, tail, None)


def spread(first, second, tips, mask, tail, with_mask):
    return pl.pallas_call(
        functools.partial(spread_kernel, with_mask),
        out_shape=jax.ShapeDtypeStruct((first.shape[0], 640 if with_mask else 512), jnp.bfloat16),
        in_specs=[VMEM] * 5,
        out_specs=VMEM,
        compiler_params=pltpu.CompilerParams(vmem_limit_bytes=9 << 20),
    )(first, second, tips, mask, tail)


def local_call(kernel, shapes, *args):
    return pl.pallas_call(
        kernel,
        out_shape=tuple(jax.ShapeDtypeStruct(shape, jnp.float32) for shape in shapes),
        in_specs=[VMEM] * len(args),
        out_specs=(VMEM,) * len(shapes),
        compiler_params=pltpu.CompilerParams(vmem_limit_bytes=9 << 20),
    )(*args)


def position():
    frame, block = lax.axis_index("frames"), lax.axis_index("blocks")
    return frame >> 4, frame & 15, block >> 3, (block >> 1) & 3, block & 1


def kept_x():
    x_lo, _, x_hi, _, _ = position()
    return x_lo == x_hi


def low_bit():
    return position()[1] & 1


def arrange_kernel(groups, *refs):
    nears, overs, refs = refs[:groups], refs[groups : 2 * groups], refs[2 * groups :]
    line_near, line_over, plain_keep, plain_send, lag_keep, lag_send = refs
    keep_near, half = kept_x(), low_bit()
    eye = lax.broadcasted_iota(jnp.int32, (128, 128), 0) == lax.broadcasted_iota(jnp.int32, (128, 128), 1)
    row = lax.broadcasted_iota(jnp.int32, (8, 256), 0)

    def wide(value):
        return jnp.broadcast_to(value, (8, value.shape[1]))

    count = wide(jnp.concatenate([line_near[128:129, 512:]] * 2, axis=1))
    lines = [[wide(ref[128:129, at : at + 256]) for at in (0, 256)] for ref in (line_near, line_over)]
    for group, (near_ref, over_ref) in enumerate(zip(nears, overs)):
        sums = jnp.sum(jnp.where(eye, near_ref[:128, 512:], 0.0), axis=0, keepdims=True)
        sums = wide(jnp.concatenate([sums, sums], axis=1))
        for out, take_near in ((plain_keep, keep_near), (plain_send, jnp.logical_not(keep_near))):
            out[group, :128, :] = jnp.where(take_near, near_ref[:128, :256], over_ref[:128, :256])
            now, later = (jnp.where(take_near, a, b) for a, b in zip(*lines))
            out[group, 128:, :] = jnp.where(row == 0, now, jnp.where(row == 1, later, jnp.where(row == 2, sums, count)))
        for out, index in ((lag_keep, half), (lag_send, 1 - half)):
            part = pl.ds(pl.multiple_of(index * LAG, LAG), LAG)
            out[group, :, :256] = near_ref[part, 256:512]
            out[group, :, 256:] = over_ref[part, 256:512]


def arrange(nears, overs, lines):
    groups = len(nears)
    shapes = [(groups, 136, 256)] * 2 + [(groups, LAG, 512)] * 2
    return local_call(functools.partial(arrange_kernel, groups), shapes, *nears, *overs, *lines)


def split_core_kernel(mine, got, keep, send_out):
    _, z, _, _, core = position()
    same = ((z >> 1) & 1) == core
    total = mine[...] + got[...]
    low, high = total[:, :, :128], total[:, :, 128:]
    keep[...] = jnp.where(same, low, high)
    send_out[...] = jnp.where(same, high, low)


def merge_plain_kernel(keep_a, got_a, keep_b, got_b, keep, send_out):
    for out, index in ((keep, low_bit()), (send_out, 1 - low_bit())):
        part = pl.ds(pl.multiple_of(index * LAG, LAG), LAG)
        for at, mine, got in ((0, keep_a, got_a), (3, keep_b, got_b)):
            for group in range(mine.shape[0]):
                out[at + group, :LAG, :] = mine[group, part, :] + got[group, part, :]
                out[at + group, LAG:, :] = mine[group, 128:, :] + got[group, 128:, :]


def merge_lag_kernel(keep_a, got_a, keep_b, got_b, keep, send_out):
    keep_near = kept_x()
    for at, mine, got in ((0, keep_a, got_a), (3, keep_b, got_b)):
        for group in range(mine.shape[0]):
            near_part = mine[group, :, :256] + got[group, :, :256]
            over_part = mine[group, :, 256:] + got[group, :, 256:]
            keep[at + group] = jnp.where(keep_near, near_part, over_part)
            send_out[at + group] = jnp.where(keep_near, over_part, near_part)


def finish_kernel(a_ref, b_ref, c_ref, d_ref, zero_ref, lag_ref):
    total = a_ref[...] + b_ref[...] + c_ref[...] + d_ref[...]
    count = total[LAG + 3 : LAG + 4, :1]
    cols, lags, line = (total[LAG + i : LAG + i + 1] / count for i in range(3))
    row = lax.broadcasted_iota(jnp.int32, (LAG, 128), 0) + low_bit() * LAG
    lane = lax.broadcasted_iota(jnp.int32, (LAG, 128), 1)
    means = jnp.sum(jnp.where(lane == row, jnp.broadcast_to(line, (LAG, 128)), 0.0), axis=1, keepdims=True)
    zero_ref[...] = total[:LAG] / count - means * cols
    lag_ref[...] = total[LAG + 8 :] / count - means * lags


def finish(parts):
    return local_call(finish_kernel, [(LAG, 128)] * 2, *parts)


def shards(frames_data, traj_ids):
    _, z, _, y, _ = position()
    z_high = z >> 2

    own = frames_data
    rows = own.shape[0]
    over_x = send(own, swap_x_hi)
    up, down = send(own, up_y), send(own, down_y)
    over_core = send(own, swap_core)
    marks = traj_ids + 1
    mark_rows = jnp.pad(marks[None, :LAG].astype(jnp.bfloat16), ((0, 15), (0, 128 - LAG)))
    tip = send(jnp.concatenate([own[:LAG], over_core[:LAG], mark_rows]), to_previous)
    near_tips = tip[: 2 * LAG]
    over_tips = send(near_tips, swap_x_hi)
    over_both = send(over_x, swap_core)
    middle = rows * 9 // 14
    up_part, down_part = up[:middle], down[middle:]
    far_a, far_b = send(up_part, up_y), send(down_part, down_y)

    def columns(valid):
        return jnp.broadcast_to(valid.astype(jnp.bfloat16)[:, None], (valid.shape[0], 128))

    mask = lax.optimization_barrier(columns(marks[LAG:] == marks[:-LAG]))
    mask_tail = lax.optimization_barrier(columns(tip[2 * LAG, :LAG].astype(jnp.int32) == marks[-LAG:]))

    near_cols = spread(own, over_core, near_tips, mask, mask_tail, True)
    over_cols = spread(over_x, over_both, over_tips, mask, mask_tail, False)
    own_ones = lax.optimization_barrier(jnp.concatenate([own, jnp.ones((rows, 8), jnp.bfloat16)], axis=1))

    sides = (own_ones, down, up)
    side_near = [contract(own_ones, near_cols)]
    side_near += [contract(left, near_cols) for left in sides[1:]]
    side_over = [contract(left, over_cols) for left in sides]
    beyond = jnp.concatenate([far_a, far_b])
    far_near, far_over = contract(beyond, near_cols), contract(beyond, over_cols)

    lines = (side_near[0], side_over[0])
    side = arrange(side_near, side_over, lines)
    far = arrange([far_near], [far_over], lines)
    plain_a, lagged_a = send(side[1], swap_x_lo), send(side[3], near(1))
    plain_b, lagged_b = send(far[1], swap_x_lo), send(far[3], near(1))

    def local(kernel, count, columns, *args):
        return local_call(kernel, [(4, count, columns)] * 2, *args)

    kept, sent = local(merge_plain_kernel, 72, 256, side[0], plain_a, far[0], plain_b)
    got = send(sent, near(1))
    kept_lag, sent = local(merge_lag_kernel, LAG, 256, side[2], lagged_a, far[2], lagged_b)
    got_lag = send(sent, swap_x_lo)
    kept, sent = local(split_core_kernel, 72, 128, kept, got)
    plain = kept + send(sent, near_shifted(2))
    kept, sent = local(split_core_kernel, LAG, 128, kept_lag, got_lag)
    lagged = kept + send(sent, near(2))
    pieces = jnp.concatenate([plain, lagged], axis=1)

    parts = []
    for move in (2, 1, 3, 0):
        away = (z_high + move - y) % 4
        piece = lax.dynamic_index_in_dim(pieces, away ^ (away // 2), 0, keepdims=False)
        parts.append(send(piece, to_owner(move)))
    return finish(parts)


def solution(mesh):
    return jax.shard_map(
        shards,
        mesh=mesh,
        in_specs=(P("frames", "blocks"), P("frames")),
        out_specs=(P("frames", "blocks"), P("frames", "blocks")),
        check_vma=False,
    )
```
